16 devices in a mesh: rep: 4 (over y, z, core), dp: 4 (over x).
Axes of the slice: x: 4, y: 2, z: 1, core: 2. Of those that a mesh axis runs over, the one named last changes fastest.
The devices are a block of a 4x4x8 slice.
Arguments:
- x: bfloat16 [16, 4096, 896], P(('rep', 'dp')), parts along dimension 0
- dy: bfloat16 [16, 4096, 896], P(('rep', 'dp')), parts along dimension 0
- w_gate: bfloat16 [2, 896, 2304], P(None, 'dp')
- w_up: bfloat16 [2, 896, 2304], P(None, 'dp')
- w_down: bfloat16 [2, 2304, 896], P(None, 'dp')
Outputs:
- output 1: bfloat16 [16, 4096, 896], P(('rep', 'dp')), parts along dimension 0
- output 2: bfloat16 [8, 896, 2304], P('rep', 'dp'), parts along dimension 0
- output 3: bfloat16 [8, 896, 2304], P('rep', 'dp'), parts along dimension 0
- output 4: bfloat16 [8, 2304, 896], P('rep', 'dp'), parts along dimension 0
There are 4 independent parts. The reference program is written for one: setup_inputs(seed, part) draws one part's arguments, and reference() takes and returns one part's arrays. A program takes and returns all parts, laid end to end along the dimension named above; an argument that names none is the same for every part.
All inputs are finite; a program needn't handle non-finite values.
Results may differ from the reference program's by a relative error of at most 0.018.
Values are sent between devices in bfloat16 or wider.
A program may use at most 768 MiB of HBM per device.

```python
import jax
import jax.numpy as jnp
from jax import lax

SEQUENCES = 4
TOKENS = 4096
D = 896
FF = 2304
LAYERS = 2
NAMES = ("w_gate", "w_up", "w_down")
SHAPES = {"w_gate": (LAYERS, D, FF), "w_up": (LAYERS, D, FF), "w_down": (LAYERS, FF, D)}


def bump(key, n, height):
    away = (jnp.arange(n, dtype=jnp.int32) - jax.random.randint(key, (), 0, n, jnp.int32)) % n
    return jnp.where(away < n // 8, height, 1.0)


def together(key, own, strength):
    shared = jax.random.normal(key, own.shape[1:], jnp.float32)
    return (own + strength * shared) * lax.rsqrt(1 + strength * strength)


def setup_inputs(seed: int = 0, part: int = 0) -> dict:
    kx, kdy, ka, kb, kz, kf, kh, kl, *kw = jax.random.split(jax.random.key(seed), 8 + len(NAMES))
    kx, kdy, ka, kb = (jax.random.fold_in(k, part) for k in (kx, kdy, ka, kb))
    shape = (SEQUENCES, TOKENS, D)
    much_x, much_dy = jax.random.uniform(kz, (2,), jnp.float32, 0.0, 1.0)
    layers = 2.0 ** jax.random.uniform(kl, (LAYERS, 1, 1), jnp.float32, -1.0, 1.0)
    x = together(ka, jax.random.normal(kx, shape, jnp.float32), much_x) * bump(kf, D, 4.0)
    dy = together(kb, jax.random.normal(kdy, shape, jnp.float32), much_dy)
    drawn = {"x": x.astype(jnp.bfloat16), "dy": (dy * (SEQUENCES * TOKENS) ** -0.5).astype(jnp.bfloat16)}
    for key, name in zip(kw, NAMES, strict=True):
        w = jax.random.normal(key, SHAPES[name], jnp.float32) * SHAPES[name][1] ** -0.5
        drawn[name] = (w * {"w_gate": 1.0, "w_up": bump(kh, FF, 4.0), "w_down": layers}[name]).astype(jnp.bfloat16)
    return drawn


def matmul(a, w):
    return jnp.dot(a, w, preferred_element_type=jnp.float32).astype(jnp.bfloat16)


def normed(h):
    wide = h.astype(jnp.float32)
    scale = lax.rsqrt(jnp.mean(wide**2, -1, keepdims=True) + 1e-6)
    return (wide * scale).astype(jnp.bfloat16)


def layer(h, w):
    a = normed(h)
    gate = jnp.dot(a, w["w_gate"], preferred_element_type=jnp.float32)
    up = jnp.dot(a, w["w_up"], preferred_element_type=jnp.float32)
    return h + matmul((jax.nn.silu(gate) * up).astype(jnp.bfloat16), w["w_down"])


def stack(weights, h):
    return lax.scan(lambda h, w: (layer(h, w), None), h, weights)[0]


def reference(x, dy, w_gate, w_up, w_down):
    weights = dict(zip(NAMES, (w_gate, w_up, w_down), strict=True))

    def take(so_far, sequence):
        h, by_y = sequence
        _, back = jax.vjp(stack, weights, h)
        by_weights, by_h = back(by_y)
        return jax.tree.map(lambda total, term: total + term.astype(jnp.float32), so_far, by_weights), by_h

    none_yet = {name: jnp.zeros(w.shape, jnp.float32) for name, w in weights.items()}
    by_weights, by_x = lax.scan(take, none_yet, (x, dy))
    return (by_x, *(by_weights[name].astype(jnp.bfloat16) for name in NAMES))
```

```python
import functools

import jax
import jax.numpy as jnp
from jax import lax
from jax.experimental import pallas as pl
from jax.experimental.pallas import tpu as pltpu
from jax.sharding import PartitionSpec as P

F32, BF16 = jnp.float32, jnp.bfloat16
ANY = pl.BlockSpec(memory_space=pl.ANY)


def nn(a, b):
    return jnp.dot(a, b, preferred_element_type=F32)


def nt(a, b):
    return lax.dot_general(a, b, (((1,), (1,)), ((), ())), preferred_element_type=F32)


def scale_of(wide):
    return lax.rsqrt(jnp.mean(wide**2, -1, keepdims=True) + 1e-6)


def sigmoid(x):
    return 1.0 / (1.0 + jnp.exp(-x))


def fetch(pairs, sems):
    copies = [pltpu.make_async_copy(source, whole, sems.at[at]) for at, (source, whole) in enumerate(pairs)]
    for c in copies:
        c.start()
    for c in copies:
        c.wait()


def chunks(width, size):
    return [slice(at, min(at + size, width)) for at in range(0, width, size)]


def params(mb=60):
    return pltpu.CompilerParams(dimension_semantics=("arbitrary",), vmem_limit_bytes=mb * 1024 * 1024)


def cost(flops, nbytes):
    return pl.CostEstimate(flops=int(flops), bytes_accessed=int(nbytes), transcendentals=0)


def rows_spec(bm, d):
    return pl.BlockSpec((bm, d), lambda i: (i, 0))


MESH = pl.DeviceIdType.MESH


class Unit:
    def __init__(self, place, whole, own, layer, columns, parts, send, recv):
        core, left, me, right, opposite, there = place
        self.whole, self.columns, self.core, self.me = whole.at[layer], columns, core, me
        self.rows = own.shape[1]
        half = self.rows // 2
        self.number = 0

        def view(owner, part):
            rows, cols = part
            at = pl.multiple_of(owner * self.rows + core * half + rows[0], 16)
            return self.whole.at[pl.ds(at, rows[1]), cols]

        def copy(source, target, to):
            at = self.number
            self.number += 1
            return pltpu.make_async_remote_copy(source, target, send.at[at], recv.at[at], device_id=there[to], device_id_type=MESH)

        everything = ((0, half), columns)
        mine = own.at[layer, pl.ds(pl.multiple_of(core * half, 16), half), columns]
        self.first = [copy(mine, view(me, everything), to) for to in ("left", "right")]
        self.onward = [copy(view(frm, part), view(frm, part), to) for frm, part, to in ((right, parts[0], "left"), (left, parts[1], "right"))]
        self.across = [copy(view(frm, everything), view(frm, everything), "partner") for frm in (right, left)]
        self.last = [copy(view(opposite, everything), view(opposite, everything), "partner")]

    def start(self):
        for c in self.first:
            c.start()

    def pump(self):
        for c, on, over in zip(self.first, self.onward, self.across, strict=True):
            c.wait_recv()
            on.start()
            over.start()

    def finish(self):
        for c in self.onward:
            c.wait_recv()
        for c in self.last:
            c.start()

    def arrived(self):
        for c in self.across + self.last:
            c.wait_recv()

    def sent(self):
        for c in self.first + self.onward + self.across + self.last:
            c.wait_send()


COPIES = 7


def forward(x, w_gate, w_up, w_down, n, bm=256, pieces=2, cw=384):
    t, d = x.shape
    layers, _, f = w_gate.shape
    width = f // pieces
    tiles = t // bm
    halves = [w_gate.shape[1] // 2, w_down.shape[1] // 2]
    units = []

    def split(columns, rows):
        size = columns.stop - columns.start
        middle = columns.start + -(-(size // 128) // 2) * 128
        return [((0, rows), slice(columns.start, middle)), ((0, rows), slice(middle, columns.stop))]

    for p in range(pieces):
        columns = slice(p * width, (p + 1) * width)
        units += [(which, 0, columns, split(columns, halves[0])) for which in (0, 1)]
    whole_d = slice(0, d)
    by_rows = [((0, halves[1] // 2), whole_d), ((halves[1] // 2, halves[1] // 2), whole_d)]
    units.append((2, 0, whole_d, by_rows))
    for layer in range(1, layers):
        whole_f = slice(0, f)
        units += [(which, layer, whole_f, split(whole_f, halves[0])) for which in (0, 1)]
        units.append((2, layer, whole_d, by_rows))
    count = len(units)

    sizes = [(u[2].stop - u[2].start) * halves[0 if u[0] < 2 else 1] * 2 / 46e3 for u in units]
    order = [("s", 0), ("s", 1), ("f", 0), ("f", 1), ("s", 2), ("s", 3)]
    for k in range(2, count):
        order.append(("f", k))
        if k + 2 < count:
            order.append(("s", k + 2))
    clock, due = 3.0, {}
    for kind, k in order:
        clock += sizes[k] * (1.0 if kind == "s" else 0.5)
        due[kind, k] = clock + 2.0
    begin = due["f", 1] + 3.0
    pace = 52.0 / (pieces * tiles)
    steps = (pieces + 1) * tiles

    def step_of(time):
        return min(max(int((time - begin) / pace) + 1, 1), steps - 1)

    need = {2 * p + w: p * tiles for p in range(pieces) for w in (0, 1)} | {2 * pieces: pieces * tiles}
    events = []
    floor = 1
    for k in range(2, count):
        floor = max(floor, min(step_of(due["s", k]), need.get(k, steps - 1)))
        events.append((floor, "pump", k))
    late = {k: max(at, min(step_of(due["f", k]), need.get(k, steps - 1))) for at, _, k in events}

    def kernel(x_ref, gs, us, ds, at_ref, g_ref, u_ref, h_ref, wg, wu, wd, hidden, vg, vu, vd, og, ou, od, local, send, recv):
        i = pl.program_id(0)
        rep, me = lax.axis_index("rep"), lax.axis_index("dp")
        core = lax.rem(rep, 2)
        other = rep + 1 - 2 * core
        left, right, opposite = lax.rem(me + n - 1, n), lax.rem(me + 1, n), lax.rem(me + 2, n)
        there = {"left": (rep, left), "right": (rep, right), "partner": (other, me)}
        place = (core, left, me, right, opposite, there)
        wholes, owns = (wg, wu, wd), (og, ou, od)
        flows = [
            Unit(place, wholes[which], owns[which], layer, columns, parts, send.at[at], recv.at[at])
            for at, (which, layer, columns, parts) in enumerate(units)
        ]
        keep = []
        for which in range(3):
            rows = owns[which].shape[1]
            for layer in range(layers):
                target = wholes[which].at[layer, pl.ds(pl.multiple_of(me * rows, 16), rows)]
                keep.append(pltpu.make_async_copy(owns[which].at[layer], target, local.at[3 + len(keep)]))

        @pl.when(i == 0)
        def _():
            fetch(((gs, og), (us, ou), (ds, od)), local)
            barrier = pltpu.get_barrier_semaphore()
            for to in there.values():
                pl.semaphore_signal(barrier, inc=1, device_id=to, device_id_type=MESH)
            pl.semaphore_wait(barrier, len(there))
            flows[0].start()
            flows[1].start()
            for c in keep:
                c.start()
            flows[0].pump()
            flows[1].pump()
            flows[2].start()
            flows[3].start()
            for c in keep:
                c.wait()
            for flow in flows[:2]:
                flow.finish()
            for flow in flows[:2]:
                flow.arrived()

        for step in range(1, steps):
            pumps = [k for at, _, k in events if at == step]
            ends = [k for k in late if late[k] == step]
            if pumps or ends:

                @pl.when(i == step)
                def _(pumps=pumps, ends=ends):
                    for k in pumps:
                        flows[k].pump()
                        if k + 2 < count:
                            flows[k + 2].start()
                    for k in ends:
                        flows[k].finish()

        for p in range(pieces):

            @pl.when(i == p * tiles)
            def _(p=p):
                if p:
                    flows[2 * p].arrived()
                    flows[2 * p + 1].arrived()
                columns = pl.ds(p * width, width)
                fetch(((wg.at[0, :, columns], vg.at[:, columns]), (wu.at[0, :, columns], vu.at[:, columns])), local)

        @pl.when(i == pieces * tiles)
        def _():
            flows[2 * pieces].arrived()
            fetch(((wd.at[0], vd),), local)

        for p in range(pieces):

            @pl.when(i // tiles == p)
            def _(p=p):
                wide = x_ref[...].astype(F32)
                a = (wide * scale_of(wide)).astype(BF16)
                if p == 0:
                    at_ref[...] = a.T
                rows = pl.ds(pl.multiple_of((i - p * tiles) * bm, bm), bm)
                for c in chunks(width, cw):
                    from_all = slice(p * width + c.start, p * width + c.stop)
                    g = nn(a, vg[:, from_all])
                    u = nn(a, vu[:, from_all])
                    g_ref[:, c] = g
                    u_ref[:, c] = u
                    hidden[rows, from_all] = (g * sigmoid(g) * u).astype(BF16)

        @pl.when(i // tiles == pieces)
        def _():
            rows = pl.ds(pl.multiple_of((i - pieces * tiles) * bm, bm), bm)
            h_ref[...] = x_ref[...] + nn(hidden[rows, :], vd[...]).astype(BF16)

        @pl.when(i == steps - 1)
        def _():
            for flow in flows[2 * pieces + 1 :]:
                flow.arrived()
            for flow in flows:
                flow.sent()

    def tile(i):
        return lax.rem(i, tiles)

    last = pieces * tiles - 1
    once = pl.BlockSpec((bm, width), lambda i: (tile(jnp.minimum(i, last)), jnp.minimum(i, last) // tiles))
    return pl.pallas_call(
        kernel,
        grid=(steps,),
        in_specs=[pl.BlockSpec((bm, d), lambda i: (tile(i), 0)), ANY, ANY, ANY],
        out_specs=[
            pl.BlockSpec((d, bm), lambda i: (0, jnp.minimum(i, tiles - 1))),
            once,
            once,
            pl.BlockSpec((bm, d), lambda i: (jnp.maximum(i - pieces * tiles, 0), 0)),
            ANY,
            ANY,
            ANY,
        ],
        out_shape=[
            jax.ShapeDtypeStruct((d, t), BF16),
            jax.ShapeDtypeStruct((t, f), F32),
            jax.ShapeDtypeStruct((t, f), F32),
            jax.ShapeDtypeStruct((t, d), BF16),
            jax.ShapeDtypeStruct((layers, d, f), BF16),
            jax.ShapeDtypeStruct((layers, d, f), BF16),
            jax.ShapeDtypeStruct((layers, f, d), BF16),
        ],
        scratch_shapes=[
            pltpu.VMEM((t, f), BF16),
            pltpu.VMEM((d, f), BF16),
            pltpu.VMEM((d, f), BF16),
            pltpu.VMEM((f, d), BF16),
            pltpu.VMEM(w_gate.shape, BF16),
            pltpu.VMEM(w_up.shape, BF16),
            pltpu.VMEM(w_down.shape, BF16),
            pltpu.SemaphoreType.DMA((3 + 3 * layers,)),
            pltpu.SemaphoreType.DMA((count, COPIES)),
            pltpu.SemaphoreType.DMA((count, COPIES)),
        ],
        compiler_params=pltpu.CompilerParams(
            dimension_semantics=("arbitrary",), vmem_limit_bytes=62 * 1024 * 1024, collective_id=0, has_side_effects=True
        ),
        cost_estimate=cost(6 * t * d * f, t * f * 8 + t * d * 8),
        name="forward",
    )(x, w_gate, w_up, w_down)


class Scatter:
    @staticmethod
    def halves(rows, columns):
        if columns // 2 % 128 == 0:
            return [(slice(0, rows), slice(0, columns // 2)), (slice(0, rows), slice(columns // 2, columns))]
        return [(slice(0, rows // 2), slice(0, columns)), (slice(rows // 2, rows), slice(0, columns))]

    @staticmethod
    def scratch(term, n):
        rows, columns = term.shape[0] // n, term.shape[1]
        r, c = Scatter.halves(rows, columns)[0]
        half = (r.stop - r.start, c.stop - c.start)
        return [
            pltpu.VMEM((6, *half), BF16),
            pltpu.VMEM((4, *half), BF16),
            pltpu.VMEM((rows, columns), BF16),
            pltpu.SemaphoreType.DMA((3,)),
            pltpu.SemaphoreType.DMA((6,)),
            pltpu.SemaphoreType.DMA((6,)),
        ]

    def __init__(self, n, term, out, came, own, mine, local, send, recv):
        rep, me = lax.axis_index("rep"), lax.axis_index("dp")
        left, right, opposite = lax.rem(me + n - 1, n), lax.rem(me + 1, n), lax.rem(me + 2, n)
        rows = term.shape[0] // n
        self.out, self.came, self.own, self.mine = out, came, own, mine
        self.parts = first, second = self.halves(rows, term.shape[1])

        def of(owner, part):
            r, c = part
            at = pl.multiple_of(owner * rows + r.start, 16)
            return term.at[pl.ds(at, r.stop - r.start), c]

        def copy(source, at, to):
            return pltpu.make_async_remote_copy(
                source, came.at[at], send.at[at], recv.at[at], device_id=(rep, to), device_id_type=MESH
            )

        self.far = [copy(of(opposite, first), 0, right), copy(of(opposite, second), 1, left)]
        self.near = [copy(of(right, second), 2, right), copy(of(left, first), 3, left)]
        self.sums = [copy(own.at[2], 4, right), copy(own.at[3], 5, left)]
        self.loads = [
            pltpu.make_async_copy(of(right, first), own.at[0], local.at[0]),
            pltpu.make_async_copy(of(left, second), own.at[1], local.at[1]),
            pltpu.make_async_copy(term.at[pl.ds(pl.multiple_of(me * rows, 16), rows)], mine, local.at[2]),
        ]

    def begin(self):
        for c in self.far:
            c.start()
        for c in self.loads:
            c.start()

    def neighbours(self):
        for c in self.near:
            c.start()

    def add(self):
        for c in self.loads:
            c.wait()
        for c in self.far:
            c.wait_recv()
        for at in (0, 1):
            self.own[2 + at] = (self.own[at].astype(F32) + self.came[at].astype(F32)).astype(BF16)

    def pass_on(self):
        for c in self.sums:
            c.start()

    def end(self):
        for c in self.near + self.sums:
            c.wait_recv()
        for part, from_left, from_right in zip(self.parts, (4, 2), (3, 5), strict=True):
            total = self.mine[part].astype(F32) + self.came[from_left].astype(F32) + self.came[from_right].astype(F32)
            self.out[part] = total.astype(BF16)
        for c in self.far + self.near + self.sums:
            c.wait_send()


SCATTER = 6


def greet(n):
    rep, me = lax.axis_index("rep"), lax.axis_index("dp")
    barrier = pltpu.get_barrier_semaphore()
    for to in (lax.rem(me + n - 1, n), lax.rem(me + 1, n)):
        pl.semaphore_signal(barrier, inc=1, device_id=(rep, to), device_id_type=MESH)
    pl.semaphore_wait(barrier, 2)


def scattering(kernel, n, terms, plan, identity, grid, in_specs, out_specs, out_shape, scratch_shapes, name, flops, nbytes):
    steps = grid[0]
    ins, outs = len(in_specs), len(out_specs)
    given = [Scatter.scratch(term, n) for term in terms]

    def whole(*refs):
        i = pl.program_id(0)
        own_in, refs = refs[:ins], refs[ins:]
        term_refs, refs = refs[: len(terms)], refs[len(terms) :]
        own_out, refs = refs[:outs], refs[outs:]
        shard_refs, refs = refs[: len(terms)], refs[len(terms) :]
        own_scratch, refs = refs[: len(scratch_shapes)], refs[len(scratch_shapes) :]
        flows = [
            Scatter(n, term, shard, *refs[at * SCATTER : (at + 1) * SCATTER])
            for at, (term, shard) in enumerate(zip(term_refs, shard_refs, strict=True))
        ]

        @pl.when(i == 0)
        def _():
            greet(n)
            for step, action, which in plan:
                if step == 0:
                    getattr(flows[which], action)()

        for step in sorted({p[0] for p in plan if p[0]}):

            @pl.when(i == step)
            def _(step=step):
                for at, action, which in plan:
                    if at == step:
                        getattr(flows[which], action)()

        kernel(*own_in, *own_out, *own_scratch)

        @pl.when(i == steps - 1)
        def _():
            for flow in flows:
                flow.end()

    shards = [(term.shape[0] // n, term.shape[1]) for term in terms]
    return lambda *operands: pl.pallas_call(
        whole,
        grid=grid,
        in_specs=list(in_specs) + [ANY] * len(terms),
        out_specs=list(out_specs) + [pl.BlockSpec(shard, lambda i: (0, 0)) for shard in shards],
        out_shape=list(out_shape) + [jax.ShapeDtypeStruct(shard, BF16) for shard in shards],
        scratch_shapes=list(scratch_shapes) + [x for one in given for x in one],
        compiler_params=pltpu.CompilerParams(
            dimension_semantics=("arbitrary",),
            vmem_limit_bytes=62 * 1024 * 1024,
            collective_id=identity,
            has_side_effects=True,
        ),
        cost_estimate=cost(flops, nbytes),
        name=name,
    )(*operands, *terms)


ONE = ((0, "begin", 0), (0, "neighbours", 0), (5, "add", 0), (6, "pass_on", 0))
TWO = (
    (0, "begin", 0), (0, "neighbours", 0), (0, "begin", 1),
    (5, "add", 0), (6, "pass_on", 0), (6, "neighbours", 1),
    (11, "add", 1), (12, "pass_on", 1),
)


def to_gates(g, u, dh):
    s = sigmoid(g)
    silu = g * s
    return (dh * u * (s + silu * (1.0 - s))).astype(BF16), (dh * silu).astype(BF16), (silu * u).astype(BF16)


def finish_down(acc, o_ref, cw=256):
    for c in chunks(acc.shape[1], cw):
        o_ref[c, :] = acc[:, c].T.astype(BF16)


def top_layer(h, dy, gate, up, down, layer, bm=512, cw=768):
    t, d = h.shape
    f = gate.shape[2]

    def kernel(h_ref, dy_ref, gw, uw, dw, at_ref, dg_ref, du_ref, o_ref, wg, wu, wd, acc, sems):
        i = pl.program_id(0)

        @pl.when(i == 0)
        def _():
            fetch(((gw.at[layer], wg), (uw.at[layer], wu), (dw.at[layer], wd)), sems)
            acc[...] = jnp.zeros_like(acc)

        wide = h_ref[...].astype(F32)
        a = (wide * scale_of(wide)).astype(BF16)
        at_ref[...] = a.T
        by = dy_ref[...]
        by_t = by.T
        for c in chunks(f, cw):
            g = nn(a, wg[:, c])
            u = nn(a, wu[:, c])
            dh = nt(by, wd[c, :]).astype(BF16).astype(F32)
            dg, du, hidden = to_gates(g, u, dh)
            dg_ref[:, c] = dg
            du_ref[:, c] = du
            acc[:, c] += nn(by_t, hidden)

        @pl.when(i == pl.num_programs(0) - 1)
        def _():
            finish_down(acc, o_ref)

    return pl.pallas_call(
        kernel,
        grid=(t // bm,),
        in_specs=[rows_spec(bm, d), rows_spec(bm, d)] + [ANY] * 3,
        out_specs=[
            pl.BlockSpec((d, bm), lambda i: (0, i)),
            rows_spec(bm, f),
            rows_spec(bm, f),
            pl.BlockSpec((f, d), lambda i: (0, 0)),
        ],
        out_shape=[
            jax.ShapeDtypeStruct((d, t), BF16),
            jax.ShapeDtypeStruct((t, f), BF16),
            jax.ShapeDtypeStruct((t, f), BF16),
            jax.ShapeDtypeStruct((f, d), BF16),
        ],
        scratch_shapes=[
            pltpu.VMEM((d, f), BF16),
            pltpu.VMEM((d, f), BF16),
            pltpu.VMEM((f, d), BF16),
            pltpu.VMEM((d, f), F32),
            pltpu.SemaphoreType.DMA((3,)),
        ],
        compiler_params=params(),
        cost_estimate=cost(8 * t * d * f, t * f * 4 + t * d * 6),
        name="top_layer",
    )(h, dy, gate, up, down)


def low_layer(n, terms, identity, g, u, dy, down, layer, bm=256, cw=768):
    t, f = g.shape
    d = dy.shape[1]

    def kernel(g_ref, u_ref, dy_ref, dw, dg_ref, du_ref, o_ref, wd, acc, sems):
        i = pl.program_id(0)

        @pl.when(i == 0)
        def _():
            fetch(((dw.at[layer], wd),), sems)
            acc[...] = jnp.zeros_like(acc)

        by = dy_ref[...]
        by_t = by.T
        for c in chunks(f, cw):
            dh = nt(by, wd[c, :]).astype(BF16).astype(F32)
            dg, du, hidden = to_gates(g_ref[:, c], u_ref[:, c], dh)
            dg_ref[:, c] = dg
            du_ref[:, c] = du
            acc[:, c] += nn(by_t, hidden)

        @pl.when(i == pl.num_programs(0) - 1)
        def _():
            finish_down(acc, o_ref)

    return scattering(
        kernel, n, terms, ONE, identity,
        grid=(t // bm,),
        in_specs=[rows_spec(bm, f), rows_spec(bm, f), rows_spec(bm, d), ANY],
        out_specs=[rows_spec(bm, f), rows_spec(bm, f), pl.BlockSpec((f, d), lambda i: (0, 0))],
        out_shape=[
            jax.ShapeDtypeStruct((t, f), BF16),
            jax.ShapeDtypeStruct((t, f), BF16),
            jax.ShapeDtypeStruct((f, d), BF16),
        ],
        scratch_shapes=[pltpu.VMEM((f, d), BF16), pltpu.VMEM((d, f), F32), pltpu.SemaphoreType.DMA((1,))],
        name="low_layer", flops=4 * t * d * f, nbytes=t * f * 12 + t * d * 2,
    )(g, u, dy, down)


def weight_grads(n, terms, identity, at, dg, du, bt=512):
    d, t = at.shape
    f = dg.shape[1]
    tiles = t // bt

    def kernel(a_ref, g_ref, u_ref, og_ref, ou_ref, acc):
        i = pl.program_id(0)
        for first, x_ref, o_ref in ((0, g_ref, og_ref), (tiles, u_ref, ou_ref)):
            last = first + tiles - 1

            @pl.when(i == first)
            def _(x_ref=x_ref):
                acc[...] = nn(a_ref[...], x_ref[...])

            @pl.when((i > first) & (i < last))
            def _(x_ref=x_ref):
                acc[...] += nn(a_ref[...], x_ref[...])

            @pl.when(i == last)
            def _(x_ref=x_ref, o_ref=o_ref):
                o_ref[...] = (acc[...] + nn(a_ref[...], x_ref[...])).astype(BF16)

    return scattering(
        kernel, n, terms, ONE, identity,
        grid=(2 * tiles,),
        in_specs=[
            pl.BlockSpec((d, bt), lambda i: (0, lax.rem(i, tiles))),
            pl.BlockSpec((bt, f), lambda i: (jnp.minimum(i, tiles - 1), 0)),
            pl.BlockSpec((bt, f), lambda i: (jnp.maximum(i - tiles, 0), 0)),
        ],
        out_specs=[pl.BlockSpec((d, f), lambda i: (0, 0))] * 2,
        out_shape=[jax.ShapeDtypeStruct((d, f), BF16)] * 2,
        scratch_shapes=[pltpu.VMEM((d, f), F32)],
        name="weight_grads", flops=4 * t * d * f, nbytes=t * f * 4 + t * d * 4 + d * f * 4,
    )(at, dg, du)


def input_grad(n, terms, plan, identity, dg, du, h, dy, gate, up, layer, bm=256):
    t, d = h.shape
    f = dg.shape[1]

    def kernel(dg_ref, du_ref, h_ref, dy_ref, gw, uw, o_ref, wg, wu, sems):
        @pl.when(pl.program_id(0) == 0)
        def _():
            fetch(((gw.at[layer], wg), (uw.at[layer], wu)), sems)

        da = (nt(dg_ref[...], wg[...]) + nt(du_ref[...], wu[...])).astype(BF16).astype(F32)
        wide = h_ref[...].astype(F32)
        scale = scale_of(wide)
        along = jnp.mean(da * wide, -1, keepdims=True)
        dh = da * scale - wide * (scale * scale * scale * along)
        o_ref[...] = dy_ref[...] + dh.astype(BF16)

    return scattering(
        kernel, n, terms, plan, identity,
        grid=(t // bm,),
        in_specs=[rows_spec(bm, f), rows_spec(bm, f), rows_spec(bm, d), rows_spec(bm, d), ANY, ANY],
        out_specs=[rows_spec(bm, d)],
        out_shape=[jax.ShapeDtypeStruct((t, d), BF16)],
        scratch_shapes=[pltpu.VMEM((d, f), BF16), pltpu.VMEM((d, f), BF16), pltpu.SemaphoreType.DMA((2,))],
        name="input_grad", flops=4 * t * d * f, nbytes=t * f * 4 + t * d * 6,
    )(dg, du, h, dy, gate, up)


def solution(mesh):
    n = mesh.shape["dp"]

    def body(x, dy, w_gate, w_up, w_down):
        shape = x.shape
        x, dy = (v.reshape(v.shape[-2:]) for v in (x, dy))
        at0, g0, u0, h1, gate, up, down = forward(x, w_gate, w_up, w_down, n)
        at1, dg1, du1, dwd1 = top_layer(h1, dy, gate, up, down, 1)
        dwg1, dwu1, down1 = weight_grads(n, [dwd1], 1, at1, dg1, du1)
        dh1, gate1 = input_grad(n, [dwg1], ONE, 2, dg1, du1, h1, dy, gate, up, 1)
        dg0, du0, dwd0, up1 = low_layer(n, [dwu1], 3, g0, u0, dh1, down, 0)
        dwg0, dwu0, down0 = weight_grads(n, [dwd0], 4, at0, dg0, du0)
        dx, gate0, up0 = input_grad(n, [dwg0, dwu0], TWO, 5, dg0, du0, x, dh1, gate, up, 0)
        return dx.reshape(shape), jnp.stack([gate0, gate1]), jnp.stack([up0, up1]), jnp.stack([down0, down1])

    seq, row = P(("rep", "dp")), P(None, "dp")
    out = P("rep", "dp")
    return jax.shard_map(
        body, mesh=mesh, in_specs=(seq, seq, row, row, row), out_specs=(seq, out, out, out), check_vma=False
    )
```

```python
import functools

import jax
import jax.numpy as jnp
from jax import lax
from jax.experimental import pallas as pl
from jax.experimental.pallas import tpu as pltpu
from jax.sharding import PartitionSpec as P

F32, BF16 = jnp.float32, jnp.bfloat16
ANY = pl.BlockSpec(memory_space=pl.ANY)


def nn(a, b):
    return jnp.dot(a, b, preferred_element_type=F32)


def nt(a, b):
    return lax.dot_general(a, b, (((1,), (1,)), ((), ())), preferred_element_type=F32)


def scale_of(wide):
    return lax.rsqrt(jnp.mean(wide**2, -1, keepdims=True) + 1e-6)


def sigmoid(x):
    return 1.0 / (1.0 + jnp.exp(-x))


def fetch(pairs, sems):
    copies = [pltpu.make_async_copy(source, whole, sems.at[at]) for at, (source, whole) in enumerate(pairs)]
    for c in copies:
        c.start()
    for c in copies:
        c.wait()


def chunks(width, size):
    return [slice(at, min(at + size, width)) for at in range(0, width, size)]


def params(mb=60):
    return pltpu.CompilerParams(dimension_semantics=("arbitrary",), vmem_limit_bytes=mb * 1024 * 1024)


def cost(flops, nbytes):
    return pl.CostEstimate(flops=int(flops), bytes_accessed=int(nbytes), transcendentals=0)


def rows_spec(bm, d):
    return pl.BlockSpec((bm, d), lambda i: (i, 0))


MESH = pl.DeviceIdType.MESH


class Unit:
    def __init__(self, place, whole, own, layer, columns, parts, send, recv):
        core, left, me, right, opposite, there = place
        self.whole, self.columns, self.core, self.me = whole.at[layer], columns, core, me
        self.rows = own.shape[1]
        half = self.rows // 2
        self.number = 0

        def view(owner, part):
            rows, cols = part
            at = pl.multiple_of(owner * self.rows + core * half + rows[0], 16)
            return self.whole.at[pl.ds(at, rows[1]), cols]

        def copy(source, target, to):
            at = self.number
            self.number += 1
            return pltpu.make_async_remote_copy(source, target, send.at[at], recv.at[at], device_id=there[to], device_id_type=MESH)

        everything = ((0, half), columns)
        mine = own.at[layer, pl.ds(pl.multiple_of(core * half, 16), half), columns]
        self.first = [copy(mine, view(me, everything), to) for to in ("left", "right")]
        self.onward = [copy(view(frm, part), view(frm, part), to) for frm, part, to in ((right, parts[0], "left"), (left, parts[1], "right"))]
        self.across = [copy(view(frm, everything), view(frm, everything), "partner") for frm in (right, left)]
        self.last = [copy(view(opposite, everything), view(opposite, everything), "partner")]

    def start(self):
        for c in self.first:
            c.start()

    def pump(self):
        for c, on, over in zip(self.first, self.onward, self.across, strict=True):
            c.wait_recv()
            on.start()
            over.start()

    def finish(self):
        for c in self.onward:
            c.wait_recv()
        for c in self.last:
            c.start()

    def arrived(self):
        for c in self.across + self.last:
            c.wait_recv()

    def sent(self):
        for c in self.first + self.onward + self.across + self.last:
            c.wait_send()


COPIES = 7


def forward(x, w_gate, w_up, w_down, n, bm=512, pieces=2, cw=1152):
    t, d = x.shape
    layers, _, f = w_gate.shape
    width = f // pieces
    tiles = t // bm
    halves = [w_gate.shape[1] // 2, w_down.shape[1] // 2]
    units = []

    def split(columns, rows):
        size = columns.stop - columns.start
        middle = columns.start + -(-(size // 128) // 2) * 128
        return [((0, rows), slice(columns.start, middle)), ((0, rows), slice(middle, columns.stop))]

    for p in range(pieces):
        columns = slice(p * width, (p + 1) * width)
        units += [(which, 0, columns, split(columns, halves[0])) for which in (0, 1)]
    whole_d = slice(0, d)
    by_rows = [((0, halves[1] // 2), whole_d), ((halves[1] // 2, halves[1] // 2), whole_d)]
    units.append((2, 0, whole_d, by_rows))
    for layer in range(1, layers):
        whole_f = slice(0, f)
        units += [(which, layer, whole_f, split(whole_f, halves[0])) for which in (0, 1)]
        units.append((2, layer, whole_d, by_rows))
    count = len(units)

    sizes = [(u[2].stop - u[2].start) * halves[0 if u[0] < 2 else 1] * 2 / 60e3 for u in units]
    order = [("s", 0), ("s", 1), ("f", 0), ("f", 1), ("s", 2), ("s", 3)]
    for k in range(2, count):
        order.append(("f", k))
        if k + 2 < count:
            order.append(("s", k + 2))
    clock, due = 3.0, {}
    for kind, k in order:
        clock += sizes[k] * (1.0 if kind == "s" else 0.5)
        due[kind, k] = clock + 2.0
    begin = due["f", 1] + 3.0
    pace = 52.0 / (pieces * tiles)
    steps = (pieces + 1) * tiles

    def step_of(time):
        return min(max(int((time - begin) / pace) + 1, 1), steps - 1)

    need = {2 * p + w: p * tiles for p in range(pieces) for w in (0, 1)} | {2 * pieces: pieces * tiles}
    events = []
    floor = 1
    for k in range(2, count):
        floor = max(floor, min(step_of(due["s", k]), need.get(k, steps - 1)))
        events.append((floor, "pump", k))
    late = {k: max(at, min(step_of(due["f", k]), need.get(k, steps - 1))) for at, _, k in events}

    def kernel(x_ref, gs, us, ds, at_ref, g_ref, u_ref, h_ref, wg, wu, wd, hidden, vg, vu, vd, og, ou, od, local, send, recv):
        i = pl.program_id(0)
        rep, me = lax.axis_index("rep"), lax.axis_index("dp")
        core = lax.rem(rep, 2)
        other = rep + 1 - 2 * core
        left, right, opposite = lax.rem(me + n - 1, n), lax.rem(me + 1, n), lax.rem(me + 2, n)
        there = {"left": (rep, left), "right": (rep, right), "partner": (other, me)}
        place = (core, left, me, right, opposite, there)
        wholes, owns = (wg, wu, wd), (og, ou, od)
        flows = [
            Unit(place, wholes[which], owns[which], layer, columns, parts, send.at[at], recv.at[at])
            for at, (which, layer, columns, parts) in enumerate(units)
        ]
        keep = []
        for which in range(3):
            rows = owns[which].shape[1]
            for layer in range(layers):
                target = wholes[which].at[layer, pl.ds(pl.multiple_of(me * rows, 16), rows)]
                keep.append(pltpu.make_async_copy(owns[which].at[layer], target, local.at[3 + len(keep)]))

        @pl.when(i == 0)
        def _():
            fetch(((gs, og), (us, ou), (ds, od)), local)
            barrier = pltpu.get_barrier_semaphore()
            for to in there.values():
                pl.semaphore_signal(barrier, inc=1, device_id=to, device_id_type=MESH)
            pl.semaphore_wait(barrier, len(there))
            flows[0].start()
            flows[1].start()
            for c in keep:
                c.start()
            flows[0].pump()
            flows[1].pump()
            flows[2].start()
            flows[3].start()
            for c in keep:
                c.wait()
            for flow in flows[:2]:
                flow.finish()
            for flow in flows[:2]:
                flow.arrived()

        for step in range(1, steps):
            pumps = [k for at, _, k in events if at == step]
            ends = [k for k in late if late[k] == step]
            if pumps or ends:

                @pl.when(i == step)
                def _(pumps=pumps, ends=ends):
                    for k in pumps:
                        flows[k].pump()
                        if k + 2 < count:
                            flows[k + 2].start()
                    for k in ends:
                        flows[k].finish()

        for p in range(pieces):

            @pl.when(i == p * tiles)
            def _(p=p):
                if p:
                    flows[2 * p].arrived()
                    flows[2 * p + 1].arrived()
                columns = pl.ds(p * width, width)
                fetch(((wg.at[0, :, columns], vg.at[:, columns]), (wu.at[0, :, columns], vu.at[:, columns])), local)

        @pl.when(i == pieces * tiles)
        def _():
            flows[2 * pieces].arrived()
            fetch(((wd.at[0], vd),), local)

        for p in range(pieces):

            @pl.when(i // tiles == p)
            def _(p=p):
                wide = x_ref[...].astype(F32)
                a = (wide * scale_of(wide)).astype(BF16)
                if p == 0:
                    at_ref[...] = a.T
                rows = pl.ds(pl.multiple_of((i - p * tiles) * bm, bm), bm)
                for c in chunks(width, cw):
                    from_all = slice(p * width + c.start, p * width + c.stop)
                    g = nn(a, vg[:, from_all])
                    u = nn(a, vu[:, from_all])
                    g_ref[:, c] = g
                    u_ref[:, c] = u
                    hidden[rows, from_all] = (g * sigmoid(g) * u).astype(BF16)

        @pl.when(i // tiles == pieces)
        def _():
            rows = pl.ds(pl.multiple_of((i - pieces * tiles) * bm, bm), bm)
            h_ref[...] = x_ref[...] + nn(hidden[rows, :], vd[...]).astype(BF16)

        @pl.when(i == steps - 1)
        def _():
            for flow in flows[2 * pieces + 1 :]:
                flow.arrived()
            for flow in flows:
                flow.sent()

    def tile(i):
        return lax.rem(i, tiles)

    last = pieces * tiles - 1
    once = pl.BlockSpec((bm, width), lambda i: (tile(jnp.minimum(i, last)), jnp.minimum(i, last) // tiles))
    return pl.pallas_call(
        kernel,
        grid=(steps,),
        in_specs=[pl.BlockSpec((bm, d), lambda i: (tile(i), 0)), ANY, ANY, ANY],
        out_specs=[
            pl.BlockSpec((d, bm), lambda i: (0, jnp.minimum(i, tiles - 1))),
            once,
            once,
            pl.BlockSpec((bm, d), lambda i: (jnp.maximum(i - pieces * tiles, 0), 0)),
            ANY,
            ANY,
            ANY,
        ],
        out_shape=[
            jax.ShapeDtypeStruct((d, t), BF16),
            jax.ShapeDtypeStruct((t, f), F32),
            jax.ShapeDtypeStruct((t, f), F32),
            jax.ShapeDtypeStruct((t, d), BF16),
            jax.ShapeDtypeStruct((layers, d, f), BF16),
            jax.ShapeDtypeStruct((layers, d, f), BF16),
            jax.ShapeDtypeStruct((layers, f, d), BF16),
        ],
        scratch_shapes=[
            pltpu.VMEM((t, f), BF16),
            pltpu.VMEM((d, f), BF16),
            pltpu.VMEM((d, f), BF16),
            pltpu.VMEM((f, d), BF16),
            pltpu.VMEM(w_gate.shape, BF16),
            pltpu.VMEM(w_up.shape, BF16),
            pltpu.VMEM(w_down.shape, BF16),
            pltpu.SemaphoreType.DMA((3 + 3 * layers,)),
            pltpu.SemaphoreType.DMA((count, COPIES)),
            pltpu.SemaphoreType.DMA((count, COPIES)),
        ],
        compiler_params=pltpu.CompilerParams(
            dimension_semantics=("arbitrary",), vmem_limit_bytes=62 * 1024 * 1024, collective_id=0, has_side_effects=True
        ),
        cost_estimate=cost(6 * t * d * f, t * f * 8 + t * d * 8),
        name="forward",
    )(x, w_gate, w_up, w_down)


class Scatter:
    @staticmethod
    def halves(rows, columns):
        if columns // 2 % 128 == 0:
            return [(slice(0, rows), slice(0, columns // 2)), (slice(0, rows), slice(columns // 2, columns))]
        return [(slice(0, rows // 2), slice(0, columns)), (slice(rows // 2, rows), slice(0, columns))]

    @staticmethod
    def scratch(shape, n, here=False):
        rows, columns = shape[0] // n, shape[1]
        r, c = Scatter.halves(rows, columns)[0]
        half = (r.stop - r.start, c.stop - c.start)
        landing = [pltpu.VMEM((6, *half), BF16), pltpu.VMEM((2, *half), BF16)]
        if not here:
            landing += [pltpu.VMEM((2, *half), BF16), pltpu.VMEM((rows, columns), BF16), pltpu.SemaphoreType.DMA((3,))]
        return landing + [pltpu.SemaphoreType.DMA((6,)), pltpu.SemaphoreType.DMA((6,))]

    def __init__(self, n, term, out, came, totals, *rest):
        *loaded, send, recv = rest
        rep, me = lax.axis_index("rep"), lax.axis_index("dp")
        left, right, opposite = lax.rem(me + n - 1, n), lax.rem(me + 1, n), lax.rem(me + 2, n)
        rows = term.shape[0] // n
        self.out, self.came, self.totals = out, came, totals
        self.parts = first, second = self.halves(rows, term.shape[1])

        def of(owner, part):
            r, c = part
            at = pl.multiple_of(owner * rows + r.start, 16)
            return term.at[pl.ds(at, r.stop - r.start), c]

        def copy(source, at, to):
            return pltpu.make_async_remote_copy(
                source, came.at[at], send.at[at], recv.at[at], device_id=(rep, to), device_id_type=MESH
            )

        self.far = [copy(of(opposite, first), 0, right), copy(of(opposite, second), 1, left)]
        self.near = [copy(of(right, second), 2, right), copy(of(left, first), 3, left)]
        self.sums = [copy(totals.at[0], 4, right), copy(totals.at[1], 5, left)]
        self.loads = []
        if loaded:
            own, mine, local = loaded
            self.mine = [mine.at[part] for part in self.parts]
            self.theirs = [own.at[0], own.at[1]]
            self.loads = [
                pltpu.make_async_copy(of(right, first), own.at[0], local.at[0]),
                pltpu.make_async_copy(of(left, second), own.at[1], local.at[1]),
                pltpu.make_async_copy(term.at[pl.ds(pl.multiple_of(me * rows, 16), rows)], mine, local.at[2]),
            ]
        else:
            self.mine = [of(me, part) for part in self.parts]
            self.theirs = [of(right, first), of(left, second)]

    def begin(self):
        for c in self.far:
            c.start()
        for c in self.loads:
            c.start()

    def neighbours(self):
        for c in self.near:
            c.start()

    def add(self):
        for c in self.loads:
            c.wait()
        for c in self.far:
            c.wait_recv()
        for at in (0, 1):
            self.totals[at] = (self.theirs[at][...].astype(F32) + self.came[at].astype(F32)).astype(BF16)

    def pass_on(self):
        for c in self.sums:
            c.start()

    def end(self):
        for c in self.near + self.sums:
            c.wait_recv()
        for part, mine, from_left, from_right in zip(self.parts, self.mine, (4, 2), (3, 5), strict=True):
            total = mine[...].astype(F32) + self.came[from_left].astype(F32) + self.came[from_right].astype(F32)
            self.out[part] = total.astype(BF16)
        for c in self.far + self.near + self.sums:
            c.wait_send()


SCATTER = 7


def greet(n):
    rep, me = lax.axis_index("rep"), lax.axis_index("dp")
    barrier = pltpu.get_barrier_semaphore()
    for to in (lax.rem(me + n - 1, n), lax.rem(me + 1, n)):
        pl.semaphore_signal(barrier, inc=1, device_id=(rep, to), device_id_type=MESH)
    pl.semaphore_wait(barrier, 2)


def scattering(kernel, n, terms, plan, identity, grid, in_specs, out_specs, out_shape, scratch_shapes, name, flops, nbytes):
    steps = grid[0]
    ins, outs = len(in_specs), len(out_specs)
    given = [Scatter.scratch(term.shape, n) for term in terms]

    def whole(*refs):
        i = pl.program_id(0)
        own_in, refs = refs[:ins], refs[ins:]
        term_refs, refs = refs[: len(terms)], refs[len(terms) :]
        own_out, refs = refs[:outs], refs[outs:]
        shard_refs, refs = refs[: len(terms)], refs[len(terms) :]
        own_scratch, refs = refs[: len(scratch_shapes)], refs[len(scratch_shapes) :]
        flows = [
            Scatter(n, term, shard, *refs[at * SCATTER : (at + 1) * SCATTER])
            for at, (term, shard) in enumerate(zip(term_refs, shard_refs, strict=True))
        ]

        @pl.when(i == 0)
        def _():
            greet(n)
            for step, action, which in plan:
                if step == 0:
                    getattr(flows[which], action)()

        for step in sorted({p[0] for p in plan if p[0]}):

            @pl.when(i == step)
            def _(step=step):
                for at, action, which in plan:
                    if at == step:
                        getattr(flows[which], action)()

        kernel(*own_in, *own_out, *own_scratch)

        @pl.when(i == steps - 1)
        def _():
            for flow in flows:
                flow.end()

    shards = [(term.shape[0] // n, term.shape[1]) for term in terms]
    return lambda *operands: pl.pallas_call(
        whole,
        grid=grid,
        in_specs=list(in_specs) + [ANY] * len(terms),
        out_specs=list(out_specs) + [pl.BlockSpec(shard, lambda i: (0, 0)) for shard in shards],
        out_shape=list(out_shape) + [jax.ShapeDtypeStruct(shard, BF16) for shard in shards],
        scratch_shapes=list(scratch_shapes) + [x for one in given for x in one],
        compiler_params=pltpu.CompilerParams(
            dimension_semantics=("arbitrary",),
            vmem_limit_bytes=62 * 1024 * 1024,
            collective_id=identity,
            has_side_effects=True,
        ),
        cost_estimate=cost(flops, nbytes),
        name=name,
    )(*operands, *terms)


ONE = ((0, "begin", 0), (0, "neighbours", 0), (5, "add", 0), (6, "pass_on", 0))

def to_gates(g, u, dh):
    s = sigmoid(g)
    silu = g * s
    return (dh * u * (s + silu * (1.0 - s))).astype(BF16), (dh * silu).astype(BF16), (silu * u).astype(BF16)


def finish_down(acc, o_ref, cw=256):
    for c in chunks(acc.shape[1], cw):
        o_ref[c, :] = acc[:, c].T.astype(BF16)


def top_layer(h, dy, gate, up, down, layer, bm=512, cw=768):
    t, d = h.shape
    f = gate.shape[2]

    def kernel(h_ref, dy_ref, gw, uw, dw, at_ref, dg_ref, du_ref, o_ref, wg, wu, wd, acc, sems):
        i = pl.program_id(0)

        @pl.when(i == 0)
        def _():
            fetch(((gw.at[layer], wg), (uw.at[layer], wu), (dw.at[layer], wd)), sems)
            acc[...] = jnp.zeros_like(acc)

        wide = h_ref[...].astype(F32)
        a = (wide * scale_of(wide)).astype(BF16)
        at_ref[...] = a.T
        by = dy_ref[...]
        by_t = by.T
        for c in chunks(f, cw):
            g = nn(a, wg[:, c])
            u = nn(a, wu[:, c])
            dh = nt(by, wd[c, :]).astype(BF16).astype(F32)
            dg, du, hidden = to_gates(g, u, dh)
            dg_ref[:, c] = dg
            du_ref[:, c] = du
            acc[:, c] += nn(by_t, hidden)

        @pl.when(i == pl.num_programs(0) - 1)
        def _():
            finish_down(acc, o_ref)

    return pl.pallas_call(
        kernel,
        grid=(t // bm,),
        in_specs=[rows_spec(bm, d), rows_spec(bm, d)] + [ANY] * 3,
        out_specs=[
            pl.BlockSpec((d, bm), lambda i: (0, i)),
            rows_spec(bm, f),
            rows_spec(bm, f),
            pl.BlockSpec((f, d), lambda i: (0, 0)),
        ],
        out_shape=[
            jax.ShapeDtypeStruct((d, t), BF16),
            jax.ShapeDtypeStruct((t, f), BF16),
            jax.ShapeDtypeStruct((t, f), BF16),
            jax.ShapeDtypeStruct((f, d), BF16),
        ],
        scratch_shapes=[
            pltpu.VMEM((d, f), BF16),
            pltpu.VMEM((d, f), BF16),
            pltpu.VMEM((f, d), BF16),
            pltpu.VMEM((d, f), F32),
            pltpu.SemaphoreType.DMA((3,)),
        ],
        compiler_params=params(),
        cost_estimate=cost(8 * t * d * f, t * f * 4 + t * d * 6),
        name="top_layer",
    )(h, dy, gate, up, down)


def low_layer(n, terms, identity, g, u, dy, down, layer, bm=256, cw=768):
    t, f = g.shape
    d = dy.shape[1]

    def kernel(g_ref, u_ref, dy_ref, dw, dg_ref, du_ref, o_ref, wd, acc, sems):
        i = pl.program_id(0)

        @pl.when(i == 0)
        def _():
            fetch(((dw.at[layer], wd),), sems)
            acc[...] = jnp.zeros_like(acc)

        by = dy_ref[...]
        by_t = by.T
        for c in chunks(f, cw):
            dh = nt(by, wd[c, :]).astype(BF16).astype(F32)
            dg, du, hidden = to_gates(g_ref[:, c], u_ref[:, c], dh)
            dg_ref[:, c] = dg
            du_ref[:, c] = du
            acc[:, c] += nn(by_t, hidden)

        @pl.when(i == pl.num_programs(0) - 1)
        def _():
            finish_down(acc, o_ref)

    return scattering(
        kernel, n, terms, ONE, identity,
        grid=(t // bm,),
        in_specs=[rows_spec(bm, f), rows_spec(bm, f), rows_spec(bm, d), ANY],
        out_specs=[rows_spec(bm, f), rows_spec(bm, f), pl.BlockSpec((f, d), lambda i: (0, 0))],
        out_shape=[
            jax.ShapeDtypeStruct((t, f), BF16),
            jax.ShapeDtypeStruct((t, f), BF16),
            jax.ShapeDtypeStruct((f, d), BF16),
        ],
        scratch_shapes=[pltpu.VMEM((f, d), BF16), pltpu.VMEM((d, f), F32), pltpu.SemaphoreType.DMA((1,))],
        name="low_layer", flops=4 * t * d * f, nbytes=t * f * 12 + t * d * 2,
    )(g, u, dy, down)


def back(n, identity, term, at, dg, du, h, dy, gate, up, layer, last, bt=512, inner=256):
    d, t = at.shape
    f = dg.shape[1]
    tiles = t // bt
    steps = 3 * tiles
    middle, low = tiles, 2 * tiles
    plan = [
        (0, "begin", 0), (0, "neighbours", 0), (5, "add", 0), (6, "pass_on", 0), (middle + 5, "end", 0),
        (middle, "begin", 1), (middle, "neighbours", 1), (low + 1, "add", 1), (low + 2, "pass_on", 1), (low + 5, "end", 1),
    ]
    if last:
        plan += [(low, "begin", 2), (low + 2, "neighbours", 2), (low + 4, "add", 2), (low + 5, "pass_on", 2)]

    def kernel(at_ref, dg_ref, du_ref, h_ref, dy_ref, gw, uw, down_term, o_ref, down_out, gate_out, up_out, *scratch):
        acc, gate_term, up_term, wg, wu, sems, out_sem, *rest = scratch
        i = pl.program_id(0)
        flows = [Scatter(n, down_term, down_out, *rest[:7]), Scatter(n, gate_term, gate_out, *rest[7:11])]
        if last:
            flows.append(Scatter(n, up_term, up_out, *rest[11:15]))
        weights = [pltpu.make_async_copy(w.at[layer], v, sems.at[at]) for at, (w, v) in enumerate(((gw, wg), (uw, wu)))]

        @pl.when(i == 0)
        def _():
            for c in weights:
                c.start()
            greet(n)

        for step in sorted({p[0] for p in plan}):

            @pl.when(i == step)
            def _(step=step):
                for when, action, which in plan:
                    if when == step:
                        getattr(flows[which], action)()

        if not last:
            out = pltpu.make_async_copy(up_term, up_out, out_sem.at[0])

            @pl.when(i == low)
            def _():
                out.start()

            @pl.when(i == steps - 1)
            def _():
                out.wait()

        for first, x_ref, whole in ((0, dg_ref, gate_term), (middle, du_ref, up_term)):

            @pl.when((i >= first) & (i < first + tiles))
            def _(first=first, x_ref=x_ref, whole=whole):
                @pl.when(i == first)
                def _():
                    acc[...] = jnp.zeros_like(acc)

                acc[...] += nn(at_ref[...], x_ref[...])

                @pl.when(i == first + tiles - 1)
                def _():
                    whole[...] = acc[...].astype(BF16)

        @pl.when(i == low)
        def _():
            for c in weights:
                c.wait()

        @pl.when(i >= low)
        def _():
            @pl.loop(0, bt // inner)
            def _(part):
                rows = pl.ds(pl.multiple_of(part * inner, inner), inner)
                da = (nt(dg_ref[rows, :], wg[...]) + nt(du_ref[rows, :], wu[...])).astype(BF16).astype(F32)
                wide = h_ref[rows, :].astype(F32)
                scale = scale_of(wide)
                along = jnp.mean(da * wide, -1, keepdims=True)
                dh = da * scale - wide * (scale * scale * scale * along)
                o_ref[rows, :] = dy_ref[rows, :] + dh.astype(BF16)

        if last:

            @pl.when(i == steps - 1)
            def _():
                flows[2].end()

    def late(i):
        return (jnp.maximum(i - low, 0), 0)

    def shard(rows, columns):
        return pl.BlockSpec((rows // n, columns), lambda i: (0, 0), pipeline_mode=pl.Buffered(1))

    scratch = [
        pltpu.VMEM((d, f), F32),
        pltpu.VMEM((d, f), BF16),
        pltpu.VMEM((d, f), BF16),
        pltpu.VMEM((d, f), BF16),
        pltpu.VMEM((d, f), BF16),
        pltpu.SemaphoreType.DMA((2,)),
        pltpu.SemaphoreType.DMA((1,)),
        *Scatter.scratch((f, d), n),
        *Scatter.scratch((d, f), n, here=True),
    ]
    if last:
        scratch += Scatter.scratch((d, f), n, here=True)
    return pl.pallas_call(
        kernel,
        grid=(steps,),
        in_specs=[
            pl.BlockSpec((d, bt), lambda i: (0, lax.rem(jnp.minimum(i, low - 1), tiles))),
            pl.BlockSpec((bt, f), lambda i: (jnp.where(i < low, jnp.minimum(i, tiles - 1), i - low), 0)),
            pl.BlockSpec((bt, f), lambda i: (jnp.where(i < low, jnp.maximum(i - middle, 0), i - low), 0)),
            pl.BlockSpec((bt, d), late),
            pl.BlockSpec((bt, d), late),
            ANY,
            ANY,
            ANY,
        ],
        out_specs=[pl.BlockSpec((bt, d), late), shard(f, d), shard(d, f), shard(d, f) if last else ANY],
        out_shape=[
            jax.ShapeDtypeStruct((t, d), BF16),
            jax.ShapeDtypeStruct((f // n, d), BF16),
            jax.ShapeDtypeStruct((d // n, f), BF16),
            jax.ShapeDtypeStruct((d // n if last else d, f), BF16),
        ],
        scratch_shapes=scratch,
        compiler_params=pltpu.CompilerParams(
            dimension_semantics=("arbitrary",),
            vmem_limit_bytes=63 * 1024 * 1024,
            collective_id=identity,
            has_side_effects=True,
        ),
        cost_estimate=cost(8 * t * d * f, t * f * 8 + t * d * 10),
        name="back",
    )(at, dg, du, h, dy, gate, up, term)


def solution(mesh):
    n = mesh.shape["dp"]

    def body(x, dy, w_gate, w_up, w_down):
        shape = x.shape
        x, dy = (v.reshape(v.shape[-2:]) for v in (x, dy))
        at0, g0, u0, h1, gate, up, down = forward(x, w_gate, w_up, w_down, n)
        at1, dg1, du1, dwd1 = top_layer(h1, dy, gate, up, down, 1)
        dh1, down1, gate1, dwu1 = back(n, 1, dwd1, at1, dg1, du1, h1, dy, gate, up, 1, False)
        dg0, du0, dwd0, up1 = low_layer(n, [dwu1], 2, g0, u0, dh1, down, 0)
        dx, down0, gate0, up0 = back(n, 3, dwd0, at0, dg0, du0, x, dh1, gate, up, 0, True)
        return dx.reshape(shape), jnp.stack([gate0, gate1]), jnp.stack([up0, up1]), jnp.stack([down0, down1])

    seq, row = P(("rep", "dp")), P(None, "dp")
    out = P("rep", "dp")
    return jax.shard_map(
        body, mesh=mesh, in_specs=(seq, seq, row, row, row), out_specs=(seq, out, out, out), check_vma=False
    )
```

```python
import functools

import jax
import jax.numpy as jnp
from jax import lax
from jax.experimental import pallas as pl
from jax.experimental.pallas import tpu as pltpu
from jax.sharding import PartitionSpec as P

F32, BF16 = jnp.float32, jnp.bfloat16
ANY = pl.BlockSpec(memory_space=pl.ANY)


def nn(a, b):
    return jnp.dot(a, b, preferred_element_type=F32)


def nt(a, b):
    return lax.dot_general(a, b, (((1,), (1,)), ((), ())), preferred_element_type=F32)


def scale_of(wide):
    return lax.rsqrt(jnp.mean(wide**2, -1, keepdims=True) + 1e-6)


def sigmoid(x):
    return 1.0 / (1.0 + jnp.exp(-x))


def fetch(pairs, sems):
    copies = [pltpu.make_async_copy(source, whole, sems.at[at]) for at, (source, whole) in enumerate(pairs)]
    for c in copies:
        c.start()
    for c in copies:
        c.wait()


def chunks(width, size):
    return [slice(at, min(at + size, width)) for at in range(0, width, size)]


def params(mb=60):
    return pltpu.CompilerParams(dimension_semantics=("arbitrary",), vmem_limit_bytes=mb * 1024 * 1024)


def cost(flops, nbytes):
    return pl.CostEstimate(flops=int(flops), bytes_accessed=int(nbytes), transcendentals=0)


def rows_spec(bm, d):
    return pl.BlockSpec((bm, d), lambda i: (i, 0))


MESH = pl.DeviceIdType.MESH


class Unit:
    def __init__(self, place, whole, own, layer, columns, parts, send, recv):
        core, left, me, right, opposite, there = place
        self.whole, self.columns, self.core, self.me = whole.at[layer], columns, core, me
        self.rows = own.shape[1]
        half = self.rows // 2
        self.number = 0

        def view(owner, part):
            rows, cols = part
            at = pl.multiple_of(owner * self.rows + core * half + rows[0], 16)
            return self.whole.at[pl.ds(at, rows[1]), cols]

        def copy(source, target, to):
            at = self.number
            self.number += 1
            return pltpu.make_async_remote_copy(source, target, send.at[at], recv.at[at], device_id=there[to], device_id_type=MESH)

        everything = ((0, half), columns)
        mine = own.at[layer, pl.ds(pl.multiple_of(core * half, 16), half), columns]
        self.first = [copy(mine, view(me, everything), to) for to in ("left", "right")]
        self.onward = [copy(view(frm, part), view(frm, part), to) for frm, part, to in ((right, parts[0], "left"), (left, parts[1], "right"))]
        self.across = [copy(view(frm, everything), view(frm, everything), "partner") for frm in (right, left)]
        self.last = [copy(view(opposite, everything), view(opposite, everything), "partner")]

    def start(self):
        for c in self.first:
            c.start()

    def pump(self):
        for c, on, over in zip(self.first, self.onward, self.across, strict=True):
            c.wait_recv()
            on.start()
            over.start()

    def finish(self):
        for c in self.onward:
            c.wait_recv()
        for c in self.last:
            c.start()

    def arrived(self):
        for c in self.across + self.last:
            c.wait_recv()

    def sent(self):
        for c in self.first + self.onward + self.across + self.last:
            c.wait_send()


COPIES = 7


def forward(x, w_gate, w_up, w_down, n, bm=512, pieces=2, cw=1152):
    t, d = x.shape
    layers, _, f = w_gate.shape
    width = f // pieces
    tiles = t // bm
    halves = [w_gate.shape[1] // 2, w_down.shape[1] // 2]
    units = []

    def split(columns, rows):
        size = columns.stop - columns.start
        middle = columns.start + -(-(size // 128) // 2) * 128
        return [((0, rows), slice(columns.start, middle)), ((0, rows), slice(middle, columns.stop))]

    for p in range(pieces):
        columns = slice(p * width, (p + 1) * width)
        units += [(which, 0, columns, split(columns, halves[0])) for which in (0, 1)]
    whole_d = slice(0, d)
    by_rows = [((0, halves[1] // 2), whole_d), ((halves[1] // 2, halves[1] // 2), whole_d)]
    units.append((2, 0, whole_d, by_rows))
    for layer in range(1, layers):
        whole_f = slice(0, f)
        units += [(which, layer, whole_f, split(whole_f, halves[0])) for which in (0, 1)]
        units.append((2, layer, whole_d, by_rows))
    count = len(units)

    sizes = [(u[2].stop - u[2].start) * halves[0 if u[0] < 2 else 1] * 2 / 60e3 for u in units]
    order = [("s", 0), ("s", 1), ("f", 0), ("f", 1), ("s", 2), ("s", 3)]
    for k in range(2, count):
        order.append(("f", k))
        if k + 2 < count:
            order.append(("s", k + 2))
    clock, due = 3.0, {}
    for kind, k in order:
        clock += sizes[k] * (1.0 if kind == "s" else 0.5)
        due[kind, k] = clock + 2.0
    begin = due["f", 1] + 3.0
    pace = 52.0 / (pieces * tiles)
    steps = (pieces + 1) * tiles

    def step_of(time):
        return min(max(int((time - begin) / pace) + 1, 1), steps - 1)

    need = {2 * p + w: p * tiles for p in range(pieces) for w in (0, 1)} | {2 * pieces: pieces * tiles}
    events = []
    floor = 1
    for k in range(2, count):
        floor = max(floor, min(step_of(due["s", k]), need.get(k, steps - 1)))
        events.append((floor, "pump", k))
    late = {k: max(at, min(step_of(due["f", k]), need.get(k, steps - 1))) for at, _, k in events}

    def kernel(x_ref, gs, us, ds, at_ref, g_ref, u_ref, h_ref, wg, wu, wd, hidden, vg, vu, vd, og, ou, od, local, send, recv):
        i = pl.program_id(0)
        rep, me = lax.axis_index("rep"), lax.axis_index("dp")
        core = lax.rem(rep, 2)
        other = rep + 1 - 2 * core
        left, right, opposite = lax.rem(me + n - 1, n), lax.rem(me + 1, n), lax.rem(me + 2, n)
        there = {"left": (rep, left), "right": (rep, right), "partner": (other, me)}
        place = (core, left, me, right, opposite, there)
        wholes, owns = (wg, wu, wd), (og, ou, od)
        flows = [
            Unit(place, wholes[which], owns[which], layer, columns, parts, send.at[at], recv.at[at])
            for at, (which, layer, columns, parts) in enumerate(units)
        ]
        keep = []
        for which in range(3):
            rows = owns[which].shape[1]
            for layer in range(layers):
                target = wholes[which].at[layer, pl.ds(pl.multiple_of(me * rows, 16), rows)]
                keep.append(pltpu.make_async_copy(owns[which].at[layer], target, local.at[3 + len(keep)]))

        @pl.when(i == 0)
        def _():
            fetch(((gs, og), (us, ou), (ds, od)), local)
            barrier = pltpu.get_barrier_semaphore()
            for to in there.values():
                pl.semaphore_signal(barrier, inc=1, device_id=to, device_id_type=MESH)
            pl.semaphore_wait(barrier, len(there))
            flows[0].start()
            flows[1].start()
            for c in keep:
                c.start()
            flows[0].pump()
            flows[1].pump()
            flows[2].start()
            flows[3].start()
            for c in keep:
                c.wait()
            for flow in flows[:2]:
                flow.finish()
            for flow in flows[:2]:
                flow.arrived()

        for step in range(1, steps):
            pumps = [k for at, _, k in events if at == step]
            ends = [k for k in late if late[k] == step]
            if pumps or ends:

                @pl.when(i == step)
                def _(pumps=pumps, ends=ends):
                    for k in pumps:
                        flows[k].pump()
                        if k + 2 < count:
                            flows[k + 2].start()
                    for k in ends:
                        flows[k].finish()

        for p in range(pieces):

            @pl.when(i == p * tiles)
            def _(p=p):
                if p:
                    flows[2 * p].arrived()
                    flows[2 * p + 1].arrived()
                columns = pl.ds(p * width, width)
                fetch(((wg.at[0, :, columns], vg.at[:, columns]), (wu.at[0, :, columns], vu.at[:, columns])), local)

        @pl.when(i == pieces * tiles)
        def _():
            flows[2 * pieces].arrived()
            fetch(((wd.at[0], vd),), local)

        @pl.when(i < pieces * tiles)
        def _():
            p = i // tiles
            wide = x_ref[...].astype(F32)
            a = (wide * scale_of(wide)).astype(BF16)

            @pl.when(i < tiles)
            def _():
                at_ref[...] = a.T

            rows = pl.ds(pl.multiple_of((i - p * tiles) * bm, bm), bm)
            for c in chunks(width, cw):
                from_all = pl.ds(pl.multiple_of(p * width + c.start, 128), c.stop - c.start)
                g = nn(a, vg[:, from_all])
                u = nn(a, vu[:, from_all])
                g_ref[:, c] = g
                u_ref[:, c] = u
                hidden[rows, from_all] = (g * sigmoid(g) * u).astype(BF16)

        @pl.when(i // tiles == pieces)
        def _():
            rows = pl.ds(pl.multiple_of((i - pieces * tiles) * bm, bm), bm)
            h_ref[...] = x_ref[...] + nn(hidden[rows, :], vd[...]).astype(BF16)

        @pl.when(i == steps - 1)
        def _():
            for flow in flows[2 * pieces + 1 :]:
                flow.arrived()
            for flow in flows:
                flow.sent()

    def tile(i):
        return lax.rem(i, tiles)

    last = pieces * tiles - 1
    once = pl.BlockSpec((bm, width), lambda i: (tile(jnp.minimum(i, last)), jnp.minimum(i, last) // tiles))
    return pl.pallas_call(
        kernel,
        grid=(steps,),
        in_specs=[pl.BlockSpec((bm, d), lambda i: (tile(i), 0)), ANY, ANY, ANY],
        out_specs=[
            pl.BlockSpec((d, bm), lambda i: (0, jnp.minimum(i, tiles - 1))),
            once,
            once,
            pl.BlockSpec((bm, d), lambda i: (jnp.maximum(i - pieces * tiles, 0), 0)),
            ANY,
            ANY,
            ANY,
        ],
        out_shape=[
            jax.ShapeDtypeStruct((d, t), BF16),
            jax.ShapeDtypeStruct((t, f), F32),
            jax.ShapeDtypeStruct((t, f), F32),
            jax.ShapeDtypeStruct((t, d), BF16),
            jax.ShapeDtypeStruct((layers, d, f), BF16),
            jax.ShapeDtypeStruct((layers, d, f), BF16),
            jax.ShapeDtypeStruct((layers, f, d), BF16),
        ],
        scratch_shapes=[
            pltpu.VMEM((t, f), BF16),
            pltpu.VMEM((d, f), BF16),
            pltpu.VMEM((d, f), BF16),
            pltpu.VMEM((f, d), BF16),
            pltpu.VMEM(w_gate.shape, BF16),
            pltpu.VMEM(w_up.shape, BF16),
            pltpu.VMEM(w_down.shape, BF16),
            pltpu.SemaphoreType.DMA((3 + 3 * layers,)),
            pltpu.SemaphoreType.DMA((count, COPIES)),
            pltpu.SemaphoreType.DMA((count, COPIES)),
        ],
        compiler_params=pltpu.CompilerParams(
            dimension_semantics=("arbitrary",), vmem_limit_bytes=62 * 1024 * 1024, collective_id=0, has_side_effects=True
        ),
        cost_estimate=cost(6 * t * d * f, t * f * 8 + t * d * 8),
        name="forward",
    )(x, w_gate, w_up, w_down)


class Scatter:
    @staticmethod
    def halves(rows, columns):
        if columns // 2 % 128 == 0:
            return [(slice(0, rows), slice(0, columns // 2)), (slice(0, rows), slice(columns // 2, columns))]
        return [(slice(0, rows // 2), slice(0, columns)), (slice(rows // 2, rows), slice(0, columns))]

    @staticmethod
    def scratch(shape, n, here=False):
        rows, columns = shape[0] // n, shape[1]
        r, c = Scatter.halves(rows, columns)[0]
        half = (r.stop - r.start, c.stop - c.start)
        landing = [pltpu.VMEM((6, *half), BF16), pltpu.VMEM((2, *half), BF16)]
        if not here:
            landing += [pltpu.VMEM((2, *half), BF16), pltpu.VMEM((rows, columns), BF16), pltpu.SemaphoreType.DMA((3,))]
        return landing + [pltpu.SemaphoreType.DMA((6,)), pltpu.SemaphoreType.DMA((6,))]

    def __init__(self, n, term, out, came, totals, *rest):
        *loaded, send, recv = rest
        rep, me = lax.axis_index("rep"), lax.axis_index("dp")
        left, right, opposite = lax.rem(me + n - 1, n), lax.rem(me + 1, n), lax.rem(me + 2, n)
        rows = term.shape[0] // n
        self.out, self.came, self.totals = out, came, totals
        self.parts = first, second = self.halves(rows, term.shape[1])

        def of(owner, part):
            r, c = part
            at = pl.multiple_of(owner * rows + r.start, 16)
            return term.at[pl.ds(at, r.stop - r.start), c]

        def copy(source, at, to):
            return pltpu.make_async_remote_copy(
                source, came.at[at], send.at[at], recv.at[at], device_id=(rep, to), device_id_type=MESH
            )

        self.far = [copy(of(opposite, first), 0, right), copy(of(opposite, second), 1, left)]
        self.near = [copy(of(right, second), 2, right), copy(of(left, first), 3, left)]
        self.sums = [copy(totals.at[0], 4, right), copy(totals.at[1], 5, left)]
        self.loads = []
        if loaded:
            own, mine, local = loaded
            self.mine = [mine.at[part] for part in self.parts]
            self.theirs = [own.at[0], own.at[1]]
            self.loads = [
                pltpu.make_async_copy(of(right, first), own.at[0], local.at[0]),
                pltpu.make_async_copy(of(left, second), own.at[1], local.at[1]),
                pltpu.make_async_copy(term.at[pl.ds(pl.multiple_of(me * rows, 16), rows)], mine, local.at[2]),
            ]
        else:
            self.mine = [of(me, part) for part in self.parts]
            self.theirs = [of(right, first), of(left, second)]

    def begin(self):
        for c in self.far:
            c.start()
        for c in self.loads:
            c.start()

    def neighbours(self):
        for c in self.near:
            c.start()

    def add(self):
        for c in self.loads:
            c.wait()
        for c in self.far:
            c.wait_recv()
        for at in (0, 1):
            self.totals[at] = (self.theirs[at][...].astype(F32) + self.came[at].astype(F32)).astype(BF16)

    def pass_on(self):
        for c in self.sums:
            c.start()

    def end(self):
        for c in self.near + self.sums:
            c.wait_recv()
        for part, mine, from_left, from_right in zip(self.parts, self.mine, (4, 2), (3, 5), strict=True):
            total = mine[...].astype(F32) + self.came[from_left].astype(F32) + self.came[from_right].astype(F32)
            self.out[part] = total.astype(BF16)
        for c in self.far + self.near + self.sums:
            c.wait_send()


SCATTER = 7


def greet(n):
    rep, me = lax.axis_index("rep"), lax.axis_index("dp")
    barrier = pltpu.get_barrier_semaphore()
    for to in (lax.rem(me + n - 1, n), lax.rem(me + 1, n)):
        pl.semaphore_signal(barrier, inc=1, device_id=(rep, to), device_id_type=MESH)
    pl.semaphore_wait(barrier, 2)


def scattering(kernel, n, terms, plan, identity, grid, in_specs, out_specs, out_shape, scratch_shapes, name, flops, nbytes):
    steps = grid[0]
    ins, outs = len(in_specs), len(out_specs)
    given = [Scatter.scratch(term.shape, n) for term in terms]

    def whole(*refs):
        i = pl.program_id(0)
        own_in, refs = refs[:ins], refs[ins:]
        term_refs, refs = refs[: len(terms)], refs[len(terms) :]
        own_out, refs = refs[:outs], refs[outs:]
        shard_refs, refs = refs[: len(terms)], refs[len(terms) :]
        own_scratch, refs = refs[: len(scratch_shapes)], refs[len(scratch_shapes) :]
        flows = [
            Scatter(n, term, shard, *refs[at * SCATTER : (at + 1) * SCATTER])
            for at, (term, shard) in enumerate(zip(term_refs, shard_refs, strict=True))
        ]

        @pl.when(i == 0)
        def _():
            greet(n)
            for step, action, which in plan:
                if step == 0:
                    getattr(flows[which], action)()

        for step in sorted({p[0] for p in plan if p[0]}):

            @pl.when(i == step)
            def _(step=step):
                for at, action, which in plan:
                    if at == step:
                        getattr(flows[which], action)()

        kernel(*own_in, *own_out, *own_scratch)

        @pl.when(i == steps - 1)
        def _():
            for flow in flows:
                flow.end()

    shards = [(term.shape[0] // n, term.shape[1]) for term in terms]
    return lambda *operands: pl.pallas_call(
        whole,
        grid=grid,
        in_specs=list(in_specs) + [ANY] * len(terms),
        out_specs=list(out_specs) + [pl.BlockSpec(shard, lambda i: (0, 0)) for shard in shards],
        out_shape=list(out_shape) + [jax.ShapeDtypeStruct(shard, BF16) for shard in shards],
        scratch_shapes=list(scratch_shapes) + [x for one in given for x in one],
        compiler_params=pltpu.CompilerParams(
            dimension_semantics=("arbitrary",),
            vmem_limit_bytes=62 * 1024 * 1024,
            collective_id=identity,
            has_side_effects=True,
        ),
        cost_estimate=cost(flops, nbytes),
        name=name,
    )(*operands, *terms)


ONE = ((0, "begin", 0), (0, "neighbours", 0), (5, "add", 0), (6, "pass_on", 0))

def to_gates(g, u, dh):
    s = sigmoid(g)
    silu = g * s
    return (dh * u * (s + silu * (1.0 - s))).astype(BF16), (dh * silu).astype(BF16), (silu * u).astype(BF16)


def finish_down(acc, o_ref, cw=256):
    @pl.loop(0, acc.shape[1] // cw)
    def _(at):
        c = pl.ds(pl.multiple_of(at * cw, cw), cw)
        o_ref[c, :] = acc[:, c].T.astype(BF16)


def top_layer(h, dy, gate, up, down, layer, bm=256, cw=2304):
    t, d = h.shape
    f = gate.shape[2]

    def kernel(h_ref, dy_ref, gw, uw, dw, at_ref, both_ref, o_ref, wg, wu, wd, acc, sems):
        i = pl.program_id(0)

        @pl.when(i == 0)
        def _():
            fetch(((gw.at[layer], wg), (uw.at[layer], wu), (dw.at[layer], wd)), sems)
            acc[...] = jnp.zeros_like(acc)

        wide = h_ref[...].astype(F32)
        a = (wide * scale_of(wide)).astype(BF16)
        at_ref[...] = a.T
        by = dy_ref[...]
        by_t = by.T
        for c in chunks(f, cw):
            g = nn(a, wg[:, c])
            u = nn(a, wu[:, c])
            dh = nt(by, wd[c, :]).astype(BF16).astype(F32)
            dg, du, hidden = to_gates(g, u, dh)
            both_ref[0, :, c] = dg
            both_ref[1, :, c] = du
            acc[:, c] += nn(by_t, hidden)

        @pl.when(i == pl.num_programs(0) - 1)
        def _():
            finish_down(acc, o_ref)

    return pl.pallas_call(
        kernel,
        grid=(t // bm,),
        in_specs=[rows_spec(bm, d), rows_spec(bm, d)] + [ANY] * 3,
        out_specs=[
            pl.BlockSpec((d, bm), lambda i: (0, i)),
            pl.BlockSpec((2, bm, f), lambda i: (0, i, 0)),
            pl.BlockSpec((f, d), lambda i: (0, 0)),
        ],
        out_shape=[
            jax.ShapeDtypeStruct((d, t), BF16),
            jax.ShapeDtypeStruct((2, t, f), BF16),
            jax.ShapeDtypeStruct((f, d), BF16),
        ],
        scratch_shapes=[
            pltpu.VMEM((d, f), BF16),
            pltpu.VMEM((d, f), BF16),
            pltpu.VMEM((f, d), BF16),
            pltpu.VMEM((d, f), F32),
            pltpu.SemaphoreType.DMA((3,)),
        ],
        compiler_params=params(),
        cost_estimate=cost(8 * t * d * f, t * f * 4 + t * d * 6),
        name="top_layer",
    )(h, dy, gate, up, down)


def low_layer(n, terms, identity, g, u, dy, down, layer, bm=256, cw=768):
    t, f = g.shape
    d = dy.shape[1]

    def kernel(g_ref, u_ref, dy_ref, dw, both_ref, o_ref, wd, acc, sems):
        i = pl.program_id(0)

        @pl.when(i == 0)
        def _():
            fetch(((dw.at[layer], wd),), sems)
            acc[...] = jnp.zeros_like(acc)

        by = dy_ref[...]
        by_t = by.T
        for c in chunks(f, cw):
            dh = nt(by, wd[c, :]).astype(BF16).astype(F32)
            dg, du, hidden = to_gates(g_ref[:, c], u_ref[:, c], dh)
            both_ref[0, :, c] = dg
            both_ref[1, :, c] = du
            acc[:, c] += nn(by_t, hidden)

        @pl.when(i == pl.num_programs(0) - 1)
        def _():
            finish_down(acc, o_ref)

    return scattering(
        kernel, n, terms, ONE, identity,
        grid=(t // bm,),
        in_specs=[rows_spec(bm, f), rows_spec(bm, f), rows_spec(bm, d), ANY],
        out_specs=[pl.BlockSpec((2, bm, f), lambda i: (0, i, 0)), pl.BlockSpec((f, d), lambda i: (0, 0))],
        out_shape=[
            jax.ShapeDtypeStruct((2, t, f), BF16),
            jax.ShapeDtypeStruct((f, d), BF16),
        ],
        scratch_shapes=[pltpu.VMEM((f, d), BF16), pltpu.VMEM((d, f), F32), pltpu.SemaphoreType.DMA((1,))],
        name="low_layer", flops=4 * t * d * f, nbytes=t * f * 12 + t * d * 2,
    )(g, u, dy, down)


def back(n, identity, term, at, both, h, dy, gate, up, layer, above=(), bt=512, inner=256):
    d, t = at.shape
    f = both.shape[2]
    last = bool(above)
    tiles = t // bt
    steps = 3 * tiles
    middle, low = tiles, 2 * tiles
    plan = [
        (0, "begin", 0), (0, "neighbours", 0), (5, "add", 0), (6, "pass_on", 0), (middle + 5, "end", 0),
        (middle, "begin", 1), (middle, "neighbours", 1), (low + 1, "add", 1), (low + 2, "pass_on", 1), (low + 5, "end", 1),
    ]
    if last:
        plan += [(low, "begin", 2), (low + 2, "neighbours", 2), (low + 4, "add", 2), (low + 5, "pass_on", 2)]

    def kernel(at_ref, dg_ref, du_ref, h_ref, dy_ref, gw, uw, down_term, *refs):
        others, (o_ref, *outs), scratch = refs[: len(above)], refs[len(above) : len(above) + 4], refs[len(above) + 4 :]
        down_out, gate_out, up_out = (o.at[layer] for o in outs) if last else outs
        acc, gate_term, up_term, wg, wu, sems, out_sem, *rest = scratch
        i = pl.program_id(0)
        flows = [Scatter(n, down_term, down_out, *rest[:7]), Scatter(n, gate_term, gate_out, *rest[7:11])]
        if last:
            flows.append(Scatter(n, up_term, up_out, *rest[11:15]))
        weights = [pltpu.make_async_copy(w.at[layer], v, sems.at[at]) for at, (w, v) in enumerate(((gw, wg), (uw, wu)))]
        weights += [pltpu.make_async_copy(o, outs[at].at[layer + 1], sems.at[2 + at]) for at, o in enumerate(others)]

        @pl.when(i == 0)
        def _():
            for c in weights:
                c.start()
            greet(n)

        for step in sorted({p[0] for p in plan}):

            @pl.when(i == step)
            def _(step=step):
                for when, action, which in plan:
                    if when == step:
                        getattr(flows[which], action)()

        if not last:
            out = pltpu.make_async_copy(up_term, up_out, out_sem.at[0])

            @pl.when(i == low)
            def _():
                out.start()

            @pl.when(i == steps - 1)
            def _():
                out.wait()

        @pl.when(i < low)
        def _():
            @pl.when(lax.rem(i, tiles) == 0)
            def _():
                acc[...] = jnp.zeros_like(acc)

            acc[...] += nn(at_ref[...], dg_ref[...])

        for step, whole in ((middle - 1, gate_term), (low - 1, up_term)):

            @pl.when(i == step)
            def _(whole=whole):
                whole[...] = acc[...].astype(BF16)

        @pl.when(i == low)
        def _():
            for c in weights:
                c.wait()

        @pl.when(i >= low)
        def _():
            @pl.loop(0, bt // inner)
            def _(part):
                rows = pl.ds(pl.multiple_of(part * inner, inner), inner)
                da = (nt(dg_ref[rows, :], wg[...]) + nt(du_ref[rows, :], wu[...])).astype(BF16).astype(F32)
                wide = h_ref[rows, :].astype(F32)
                scale = scale_of(wide)
                along = jnp.mean(da * wide, -1, keepdims=True)
                dh = da * scale - wide * (scale * scale * scale * along)
                o_ref[rows, :] = dy_ref[rows, :] + dh.astype(BF16)

        if last:

            @pl.when(i == steps - 1)
            def _():
                flows[2].end()

    def late(i):
        return (jnp.maximum(i - low, 0), 0)

    def shard(rows, columns):
        if last:
            return pl.BlockSpec((2, rows // n, columns), lambda i: (0, 0, 0), pipeline_mode=pl.Buffered(1))
        return pl.BlockSpec((rows // n, columns), lambda i: (0, 0), pipeline_mode=pl.Buffered(1))

    pair = (2,) if last else ()

    scratch = [
        pltpu.VMEM((d, f), F32),
        pltpu.VMEM((d, f), BF16),
        pltpu.VMEM((d, f), BF16),
        pltpu.VMEM((d, f), BF16),
        pltpu.VMEM((d, f), BF16),
        pltpu.SemaphoreType.DMA((5,)),
        pltpu.SemaphoreType.DMA((1,)),
        *Scatter.scratch((f, d), n),
        *Scatter.scratch((d, f), n, here=True),
    ]
    if last:
        scratch += Scatter.scratch((d, f), n, here=True)
    return pl.pallas_call(
        kernel,
        grid=(steps,),
        in_specs=[
            pl.BlockSpec((d, bt), lambda i: (0, lax.rem(jnp.minimum(i, low - 1), tiles))),
            pl.BlockSpec(
                (None, bt, f),
                lambda i: (jnp.where(i < low, i // tiles, 0), jnp.where(i < low, lax.rem(i, tiles), i - low), 0),
            ),
            pl.BlockSpec((None, bt, f), lambda i: (1, jnp.maximum(i - low, 0), 0)),
            pl.BlockSpec((bt, d), late),
            pl.BlockSpec((bt, d), late),
            ANY,
            ANY,
            ANY,
            *[ANY] * len(above),
        ],
        out_specs=[pl.BlockSpec((bt, d), late), shard(f, d), shard(d, f), shard(d, f) if last else ANY],
        out_shape=[
            jax.ShapeDtypeStruct((t, d), BF16),
            jax.ShapeDtypeStruct((*pair, f // n, d), BF16),
            jax.ShapeDtypeStruct((*pair, d // n, f), BF16),
            jax.ShapeDtypeStruct((*pair, d // n if last else d, f), BF16),
        ],
        scratch_shapes=scratch,
        compiler_params=pltpu.CompilerParams(
            dimension_semantics=("arbitrary",),
            vmem_limit_bytes=63 * 1024 * 1024,
            collective_id=identity,
            has_side_effects=True,
        ),
        cost_estimate=cost(8 * t * d * f, t * f * 8 + t * d * 10),
        name="back",
    )(at, both, both, h, dy, gate, up, term, *above)


def solution(mesh):
    n = mesh.shape["dp"]

    def body(x, dy, w_gate, w_up, w_down):
        shape = x.shape
        x, dy = (v.reshape(v.shape[-2:]) for v in (x, dy))
        at0, g0, u0, h1, gate, up, down = forward(x, w_gate, w_up, w_down, n)
        at1, both1, dwd1 = top_layer(h1, dy, gate, up, down, 1)
        dh1, down1, gate1, dwu1 = back(n, 1, dwd1, at1, both1, h1, dy, gate, up, 1)
        both0, dwd0, up1 = low_layer(n, [dwu1], 2, g0, u0, dh1, down, 0)
        dx, downs, gates, ups = back(n, 3, dwd0, at0, both0, x, dh1, gate, up, 0, (down1, gate1, up1))
        return dx.reshape(shape), gates, ups, downs

    seq, row = P(("rep", "dp")), P(None, "dp")
    out = P("rep", "dp")
    return jax.shard_map(
        body, mesh=mesh, in_specs=(seq, seq, row, row, row), out_specs=(seq, out, out, out), check_vma=False
    )
```

```python
import functools

import jax
import jax.numpy as jnp
from jax import lax
from jax.experimental import pallas as pl
from jax.experimental.pallas import tpu as pltpu
from jax.sharding import PartitionSpec as P

F32, BF16 = jnp.float32, jnp.bfloat16
ANY = pl.BlockSpec(memory_space=pl.ANY)


def nn(a, b):
    return jnp.dot(a, b, preferred_element_type=F32)


def nt(a, b):
    return lax.dot_general(a, b, (((1,), (1,)), ((), ())), preferred_element_type=F32)


def scale_of(wide):
    return lax.rsqrt(jnp.mean(wide**2, -1, keepdims=True) + 1e-6)


def sigmoid(x):
    return 1.0 / (1.0 + jnp.exp(-x))


def fetch(pairs, sems):
    copies = [pltpu.make_async_copy(source, whole, sems.at[at]) for at, (source, whole) in enumerate(pairs)]
    for c in copies:
        c.start()
    for c in copies:
        c.wait()


def chunks(width, size):
    return [slice(at, min(at + size, width)) for at in range(0, width, size)]


def params(mb=60):
    return pltpu.CompilerParams(dimension_semantics=("arbitrary",), vmem_limit_bytes=mb * 1024 * 1024)


def cost(flops, nbytes):
    return pl.CostEstimate(flops=int(flops), bytes_accessed=int(nbytes), transcendentals=0)


def rows_spec(bm, d):
    return pl.BlockSpec((bm, d), lambda i: (i, 0))


MESH = pl.DeviceIdType.MESH


class Unit:
    def __init__(self, place, whole, own, layer, columns, parts, send, recv):
        core, left, me, right, opposite, there = place
        self.whole, self.columns, self.core, self.me = whole.at[layer], columns, core, me
        self.rows = own.shape[1]
        half = self.rows // 2
        self.number = 0

        def view(owner, part):
            rows, cols = part
            at = pl.multiple_of(owner * self.rows + core * half + rows[0], 16)
            return self.whole.at[pl.ds(at, rows[1]), cols]

        def copy(source, target, to):
            at = self.number
            self.number += 1
            return pltpu.make_async_remote_copy(source, target, send.at[at], recv.at[at], device_id=there[to], device_id_type=MESH)

        everything = ((0, half), columns)
        mine = own.at[layer, pl.ds(pl.multiple_of(core * half, 16), half), columns]
        self.first = [copy(mine, view(me, everything), to) for to in ("left", "right")]
        self.onward = [copy(view(frm, part), view(frm, part), to) for frm, part, to in ((right, parts[0], "left"), (left, parts[1], "right"))]
        self.across = [copy(view(frm, everything), view(frm, everything), "partner") for frm in (right, left)]
        self.last = [copy(view(opposite, everything), view(opposite, everything), "partner")]

    def start(self):
        for c in self.first:
            c.start()

    def pump(self):
        for c, on, over in zip(self.first, self.onward, self.across, strict=True):
            c.wait_recv()
            on.start()
            over.start()

    def finish(self):
        for c in self.onward:
            c.wait_recv()
        for c in self.last:
            c.start()

    def arrived(self):
        for c in self.across + self.last:
            c.wait_recv()

    def sent(self):
        for c in self.first + self.onward + self.across + self.last:
            c.wait_send()


COPIES = 7


def forward(x, w_gate, w_up, w_down, n, bm=512, pieces=2, cw=1152):
    t, d = x.shape
    layers, _, f = w_gate.shape
    width = f // pieces
    tiles = t // bm
    halves = [w_gate.shape[1] // 2, w_down.shape[1] // 2]
    units = []

    def split(columns, rows):
        size = columns.stop - columns.start
        middle = columns.start + -(-(size // 128) // 2) * 128
        return [((0, rows), slice(columns.start, middle)), ((0, rows), slice(middle, columns.stop))]

    for p in range(pieces):
        columns = slice(p * width, (p + 1) * width)
        units += [(which, 0, columns, split(columns, halves[0])) for which in (0, 1)]
    whole_d = slice(0, d)
    by_rows = [((0, halves[1] // 2), whole_d), ((halves[1] // 2, halves[1] // 2), whole_d)]
    units.append((2, 0, whole_d, by_rows))
    for layer in range(1, layers):
        whole_f = slice(0, f)
        units += [(which, layer, whole_f, split(whole_f, halves[0])) for which in (0, 1)]
        units.append((2, layer, whole_d, by_rows))
    count = len(units)

    sizes = [(u[2].stop - u[2].start) * halves[0 if u[0] < 2 else 1] * 2 / 53e3 for u in units]
    order = [("s", 0), ("s", 1), ("f", 0), ("f", 1), ("s", 2), ("s", 3)]
    for k in range(2, count):
        order.append(("f", k))
        if k + 2 < count:
            order.append(("s", k + 2))
    clock, due = 3.0, {}
    for kind, k in order:
        clock += sizes[k] * (1.0 if kind == "s" else 0.5)
        due[kind, k] = clock + 2.0
    begin = due["f", 1] + 3.0
    pace = 52.0 / (pieces * tiles)
    steps = (pieces + 1) * tiles

    def step_of(time):
        return min(max(int((time - begin) / pace) + 1, 1), steps - 1)

    need = {2 * p + w: p * tiles for p in range(pieces) for w in (0, 1)} | {2 * pieces: pieces * tiles}
    events = []
    floor = 1
    for k in range(2, count):
        floor = max(floor, min(step_of(due["s", k]), need.get(k, steps - 1)))
        events.append((floor, "pump", k))
    late = {k: max(at, min(step_of(due["f", k]), need.get(k, steps - 1))) for at, _, k in events}

    def kernel(x_ref, gs, us, ds, at_ref, g_ref, u_ref, h_ref, wg, wu, wd, hidden, vg, vu, vd, og, ou, od, local, send, recv):
        i = pl.program_id(0)
        rep, me = lax.axis_index("rep"), lax.axis_index("dp")
        core = lax.rem(rep, 2)
        other = rep + 1 - 2 * core
        left, right, opposite = lax.rem(me + n - 1, n), lax.rem(me + 1, n), lax.rem(me + 2, n)
        there = {"left": (rep, left), "right": (rep, right), "partner": (other, me)}
        place = (core, left, me, right, opposite, there)
        wholes, owns = (wg, wu, wd), (og, ou, od)
        flows = [
            Unit(place, wholes[which], owns[which], layer, columns, parts, send.at[at], recv.at[at])
            for at, (which, layer, columns, parts) in enumerate(units)
        ]
        keep = []
        for which in range(3):
            rows = owns[which].shape[1]
            for layer in range(layers):
                target = wholes[which].at[layer, pl.ds(pl.multiple_of(me * rows, 16), rows)]
                keep.append(pltpu.make_async_copy(owns[which].at[layer], target, local.at[3 + len(keep)]))

        @pl.when(i == 0)
        def _():
            fetch(((gs, og), (us, ou), (ds, od)), local)
            barrier = pltpu.get_barrier_semaphore()
            for to in there.values():
                pl.semaphore_signal(barrier, inc=1, device_id=to, device_id_type=MESH)
            pl.semaphore_wait(barrier, len(there))
            flows[0].start()
            flows[1].start()
            for c in keep:
                c.start()
            flows[0].pump()
            flows[1].pump()
            flows[2].start()
            flows[3].start()
            for c in keep:
                c.wait()
            for flow in flows[:2]:
                flow.finish()
            for flow in flows[:2]:
                flow.arrived()

        for step in range(1, steps):
            pumps = [k for at, _, k in events if at == step]
            ends = [k for k in late if late[k] == step]
            if pumps or ends:

                @pl.when(i == step)
                def _(pumps=pumps, ends=ends):
                    for k in pumps:
                        flows[k].pump()
                        if k + 2 < count:
                            flows[k + 2].start()
                    for k in ends:
                        flows[k].finish()

        for p in range(pieces):

            @pl.when(i == p * tiles)
            def _(p=p):
                if p:
                    flows[2 * p].arrived()
                    flows[2 * p + 1].arrived()
                columns = pl.ds(p * width, width)
                fetch(((wg.at[0, :, columns], vg.at[:, columns]), (wu.at[0, :, columns], vu.at[:, columns])), local)

        @pl.when(i == pieces * tiles)
        def _():
            flows[2 * pieces].arrived()
            fetch(((wd.at[0], vd),), local)

        @pl.when(i < pieces * tiles)
        def _():
            p = i // tiles
            wide = x_ref[...].astype(F32)
            a = (wide * scale_of(wide)).astype(BF16)

            @pl.when(i < tiles)
            def _():
                at_ref[...] = a.T

            rows = pl.ds(pl.multiple_of((i - p * tiles) * bm, bm), bm)
            for c in chunks(width, cw):
                from_all = pl.ds(pl.multiple_of(p * width + c.start, 128), c.stop - c.start)
                g = nn(a, vg[:, from_all])
                u = nn(a, vu[:, from_all])
                g_ref[:, c] = g
                u_ref[:, c] = u
                hidden[rows, from_all] = (g * sigmoid(g) * u).astype(BF16)

        @pl.when(i // tiles == pieces)
        def _():
            rows = pl.ds(pl.multiple_of((i - pieces * tiles) * bm, bm), bm)
            h_ref[...] = x_ref[...] + nn(hidden[rows, :], vd[...]).astype(BF16)

        @pl.when(i == steps - 1)
        def _():
            for flow in flows[2 * pieces + 1 :]:
                flow.arrived()
            for flow in flows:
                flow.sent()

    def tile(i):
        return lax.rem(i, tiles)

    last = pieces * tiles - 1
    once = pl.BlockSpec((bm, width), lambda i: (tile(jnp.minimum(i, last)), jnp.minimum(i, last) // tiles))
    return pl.pallas_call(
        kernel,
        grid=(steps,),
        in_specs=[pl.BlockSpec((bm, d), lambda i: (tile(i), 0)), ANY, ANY, ANY],
        out_specs=[
            pl.BlockSpec((d, bm), lambda i: (0, jnp.minimum(i, tiles - 1))),
            once,
            once,
            pl.BlockSpec((bm, d), lambda i: (jnp.maximum(i - pieces * tiles, 0), 0)),
            ANY,
            ANY,
            ANY,
        ],
        out_shape=[
            jax.ShapeDtypeStruct((d, t), BF16),
            jax.ShapeDtypeStruct((t, f), F32),
            jax.ShapeDtypeStruct((t, f), F32),
            jax.ShapeDtypeStruct((t, d), BF16),
            jax.ShapeDtypeStruct((layers, d, f), BF16),
            jax.ShapeDtypeStruct((layers, d, f), BF16),
            jax.ShapeDtypeStruct((layers, f, d), BF16),
        ],
        scratch_shapes=[
            pltpu.VMEM((t, f), BF16),
            pltpu.VMEM((d, f), BF16),
            pltpu.VMEM((d, f), BF16),
            pltpu.VMEM((f, d), BF16),
            pltpu.VMEM(w_gate.shape, BF16),
            pltpu.VMEM(w_up.shape, BF16),
            pltpu.VMEM(w_down.shape, BF16),
            pltpu.SemaphoreType.DMA((3 + 3 * layers,)),
            pltpu.SemaphoreType.DMA((count, COPIES)),
            pltpu.SemaphoreType.DMA((count, COPIES)),
        ],
        compiler_params=pltpu.CompilerParams(
            dimension_semantics=("arbitrary",), vmem_limit_bytes=62 * 1024 * 1024, collective_id=0, has_side_effects=True
        ),
        cost_estimate=cost(6 * t * d * f, t * f * 8 + t * d * 8),
        name="forward",
    )(x, w_gate, w_up, w_down)


class Scatter:
    @staticmethod
    def halves(rows, columns):
        if columns // 2 % 128 == 0:
            return [(slice(0, rows), slice(0, columns // 2)), (slice(0, rows), slice(columns // 2, columns))]
        return [(slice(0, rows // 2), slice(0, columns)), (slice(rows // 2, rows), slice(0, columns))]

    @staticmethod
    def scratch(shape, n, here=False):
        rows, columns = shape[0] // n, shape[1]
        r, c = Scatter.halves(rows, columns)[0]
        half = (r.stop - r.start, c.stop - c.start)
        landing = [pltpu.VMEM((6, *half), BF16), pltpu.VMEM((2, *half), BF16)]
        if not here:
            landing += [pltpu.VMEM((2, *half), BF16), pltpu.VMEM((rows, columns), BF16), pltpu.SemaphoreType.DMA((3,))]
        return landing + [pltpu.SemaphoreType.DMA((6,)), pltpu.SemaphoreType.DMA((6,))]

    def __init__(self, n, term, out, came, totals, *rest):
        *loaded, send, recv = rest
        rep, me = lax.axis_index("rep"), lax.axis_index("dp")
        left, right, opposite = lax.rem(me + n - 1, n), lax.rem(me + 1, n), lax.rem(me + 2, n)
        rows = term.shape[0] // n
        self.out, self.came, self.totals = out, came, totals
        self.parts = first, second = self.halves(rows, term.shape[1])

        def of(owner, part):
            r, c = part
            at = pl.multiple_of(owner * rows + r.start, 16)
            return term.at[pl.ds(at, r.stop - r.start), c]

        def copy(source, at, to):
            return pltpu.make_async_remote_copy(
                source, came.at[at], send.at[at], recv.at[at], device_id=(rep, to), device_id_type=MESH
            )

        self.far = [copy(of(opposite, first), 0, right), copy(of(opposite, second), 1, left)]
        self.near = [copy(of(right, second), 2, right), copy(of(left, first), 3, left)]
        self.sums = [copy(totals.at[0], 4, right), copy(totals.at[1], 5, left)]
        self.loads = []
        if loaded:
            own, mine, local = loaded
            self.mine = [mine.at[part] for part in self.parts]
            self.theirs = [own.at[0], own.at[1]]
            self.loads = [
                pltpu.make_async_copy(of(right, first), own.at[0], local.at[0]),
                pltpu.make_async_copy(of(left, second), own.at[1], local.at[1]),
                pltpu.make_async_copy(term.at[pl.ds(pl.multiple_of(me * rows, 16), rows)], mine, local.at[2]),
            ]
        else:
            self.mine = [of(me, part) for part in self.parts]
            self.theirs = [of(right, first), of(left, second)]

    def begin(self):
        for c in self.far:
            c.start()
        for c in self.loads:
            c.start()

    def neighbours(self):
        for c in self.near:
            c.start()

    def add(self):
        for c in self.loads:
            c.wait()
        for c in self.far:
            c.wait_recv()
        for at in (0, 1):
            self.totals[at] = (self.theirs[at][...].astype(F32) + self.came[at].astype(F32)).astype(BF16)

    def pass_on(self):
        for c in self.sums:
            c.start()

    def end(self):
        for c in self.near + self.sums:
            c.wait_recv()
        for part, mine, from_left, from_right in zip(self.parts, self.mine, (4, 2), (3, 5), strict=True):
            total = mine[...].astype(F32) + self.came[from_left].astype(F32) + self.came[from_right].astype(F32)
            self.out[part] = total.astype(BF16)
        for c in self.far + self.near + self.sums:
            c.wait_send()


SCATTER = 7


def greet(n):
    rep, me = lax.axis_index("rep"), lax.axis_index("dp")
    barrier = pltpu.get_barrier_semaphore()
    for to in (lax.rem(me + n - 1, n), lax.rem(me + 1, n)):
        pl.semaphore_signal(barrier, inc=1, device_id=(rep, to), device_id_type=MESH)
    pl.semaphore_wait(barrier, 2)


def scattering(kernel, n, terms, plan, identity, grid, in_specs, out_specs, out_shape, scratch_shapes, name, flops, nbytes):
    steps = grid[0]
    ins, outs = len(in_specs), len(out_specs)
    given = [Scatter.scratch(term.shape, n) for term in terms]

    def whole(*refs):
        i = pl.program_id(0)
        own_in, refs = refs[:ins], refs[ins:]
        term_refs, refs = refs[: len(terms)], refs[len(terms) :]
        own_out, refs = refs[:outs], refs[outs:]
        shard_refs, refs = refs[: len(terms)], refs[len(terms) :]
        own_scratch, refs = refs[: len(scratch_shapes)], refs[len(scratch_shapes) :]
        flows = [
            Scatter(n, term, shard, *refs[at * SCATTER : (at + 1) * SCATTER])
            for at, (term, shard) in enumerate(zip(term_refs, shard_refs, strict=True))
        ]

        @pl.when(i == 0)
        def _():
            greet(n)
            for step, action, which in plan:
                if step == 0:
                    getattr(flows[which], action)()

        for step in sorted({p[0] for p in plan if p[0]}):

            @pl.when(i == step)
            def _(step=step):
                for at, action, which in plan:
                    if at == step:
                        getattr(flows[which], action)()

        kernel(*own_in, *own_out, *own_scratch)

        @pl.when(i == steps - 1)
        def _():
            for flow in flows:
                flow.end()

    shards = [(term.shape[0] // n, term.shape[1]) for term in terms]
    return lambda *operands: pl.pallas_call(
        whole,
        grid=grid,
        in_specs=list(in_specs) + [ANY] * len(terms),
        out_specs=list(out_specs) + [pl.BlockSpec(shard, lambda i: (0, 0)) for shard in shards],
        out_shape=list(out_shape) + [jax.ShapeDtypeStruct(shard, BF16) for shard in shards],
        scratch_shapes=list(scratch_shapes) + [x for one in given for x in one],
        compiler_params=pltpu.CompilerParams(
            dimension_semantics=("arbitrary",),
            vmem_limit_bytes=62 * 1024 * 1024,
            collective_id=identity,
            has_side_effects=True,
        ),
        cost_estimate=cost(flops, nbytes),
        name=name,
    )(*operands, *terms)


ONE = ((0, "begin", 0), (0, "neighbours", 0), (5, "add", 0), (6, "pass_on", 0))

def to_gates(g, u, dh):
    s = sigmoid(g)
    silu = g * s
    return (dh * u * (s + silu * (1.0 - s))).astype(BF16), (dh * silu).astype(BF16), (silu * u).astype(BF16)


def finish_down(acc, o_ref, cw=256):
    @pl.loop(0, acc.shape[1] // cw)
    def _(at):
        c = pl.ds(pl.multiple_of(at * cw, cw), cw)
        o_ref[c, :] = acc[:, c].T.astype(BF16)


def top_layer(h, dy, gate, up, down, layer, bm=256, cw=2304):
    t, d = h.shape
    f = gate.shape[2]

    def kernel(h_ref, dy_ref, gw, uw, dw, at_ref, both_ref, o_ref, wg, wu, wd, acc, sems):
        i = pl.program_id(0)

        @pl.when(i == 0)
        def _():
            fetch(((gw.at[layer], wg), (uw.at[layer], wu), (dw.at[layer], wd)), sems)
            acc[...] = jnp.zeros_like(acc)

        wide = h_ref[...].astype(F32)
        a = (wide * scale_of(wide)).astype(BF16)
        at_ref[...] = a.T
        by = dy_ref[...]
        by_t = by.T
        for c in chunks(f, cw):
            g = nn(a, wg[:, c])
            u = nn(a, wu[:, c])
            dh = nt(by, wd[c, :]).astype(BF16).astype(F32)
            dg, du, hidden = to_gates(g, u, dh)
            both_ref[0, :, c] = dg
            both_ref[1, :, c] = du
            acc[:, c] += nn(by_t, hidden)

        @pl.when(i == pl.num_programs(0) - 1)
        def _():
            finish_down(acc, o_ref)

    return pl.pallas_call(
        kernel,
        grid=(t // bm,),
        in_specs=[rows_spec(bm, d), rows_spec(bm, d)] + [ANY] * 3,
        out_specs=[
            pl.BlockSpec((d, bm), lambda i: (0, i)),
            pl.BlockSpec((2, bm, f), lambda i: (0, i, 0)),
            pl.BlockSpec((f, d), lambda i: (0, 0)),
        ],
        out_shape=[
            jax.ShapeDtypeStruct((d, t), BF16),
            jax.ShapeDtypeStruct((2, t, f), BF16),
            jax.ShapeDtypeStruct((f, d), BF16),
        ],
        scratch_shapes=[
            pltpu.VMEM((d, f), BF16),
            pltpu.VMEM((d, f), BF16),
            pltpu.VMEM((f, d), BF16),
            pltpu.VMEM((d, f), F32),
            pltpu.SemaphoreType.DMA((3,)),
        ],
        compiler_params=params(),
        cost_estimate=cost(8 * t * d * f, t * f * 4 + t * d * 6),
        name="top_layer",
    )(h, dy, gate, up, down)


def low_layer(n, terms, identity, g, u, dy, down, layer, bm=256, cw=768):
    t, f = g.shape
    d = dy.shape[1]

    def kernel(g_ref, u_ref, dy_ref, dw, both_ref, o_ref, wd, acc, sems):
        i = pl.program_id(0)

        @pl.when(i == 0)
        def _():
            fetch(((dw.at[layer], wd),), sems)
            acc[...] = jnp.zeros_like(acc)

        by = dy_ref[...]
        by_t = by.T
        for c in chunks(f, cw):
            dh = nt(by, wd[c, :]).astype(BF16).astype(F32)
            dg, du, hidden = to_gates(g_ref[:, c], u_ref[:, c], dh)
            both_ref[0, :, c] = dg
            both_ref[1, :, c] = du
            acc[:, c] += nn(by_t, hidden)

        @pl.when(i == pl.num_programs(0) - 1)
        def _():
            finish_down(acc, o_ref)

    return scattering(
        kernel, n, terms, ONE, identity,
        grid=(t // bm,),
        in_specs=[rows_spec(bm, f), rows_spec(bm, f), rows_spec(bm, d), ANY],
        out_specs=[pl.BlockSpec((2, bm, f), lambda i: (0, i, 0)), pl.BlockSpec((f, d), lambda i: (0, 0))],
        out_shape=[
            jax.ShapeDtypeStruct((2, t, f), BF16),
            jax.ShapeDtypeStruct((f, d), BF16),
        ],
        scratch_shapes=[pltpu.VMEM((f, d), BF16), pltpu.VMEM((d, f), F32), pltpu.SemaphoreType.DMA((1,))],
        name="low_layer", flops=4 * t * d * f, nbytes=t * f * 12 + t * d * 2,
    )(g, u, dy, down)


def back(n, identity, term, at, both, h, dy, gate, up, layer, above=(), bt=512, inner=256):
    d, t = at.shape
    f = both.shape[2]
    last = bool(above)
    tiles = t // bt
    steps = 3 * tiles
    middle, low = tiles, 2 * tiles
    plan = [
        (0, "begin", 0), (0, "neighbours", 0), (5, "add", 0), (6, "pass_on", 0), (middle + 5, "end", 0),
        (middle, "begin", 1), (middle, "neighbours", 1), (low + 1, "add", 1), (low + 2, "pass_on", 1), (low + 5, "end", 1),
    ]
    if last:
        plan += [(low, "begin", 2), (low + 2, "neighbours", 2), (low + 4, "add", 2), (low + 5, "pass_on", 2)]

    def kernel(at_ref, dg_ref, du_ref, h_ref, dy_ref, gw, uw, down_term, *refs):
        others, (o_ref, *outs), scratch = refs[: len(above)], refs[len(above) : len(above) + 4], refs[len(above) + 4 :]
        down_out, gate_out, up_out = (o.at[layer] for o in outs) if last else outs
        acc, gate_term, up_term, wg, wu, sems, out_sem, *rest = scratch
        i = pl.program_id(0)
        flows = [Scatter(n, down_term, down_out, *rest[:7]), Scatter(n, gate_term, gate_out, *rest[7:11])]
        if last:
            flows.append(Scatter(n, up_term, up_out, *rest[11:15]))
        weights = [pltpu.make_async_copy(w.at[layer], v, sems.at[at]) for at, (w, v) in enumerate(((gw, wg), (uw, wu)))]
        weights += [pltpu.make_async_copy(o, outs[at].at[layer + 1], sems.at[2 + at]) for at, o in enumerate(others)]

        @pl.when(i == 0)
        def _():
            for c in weights:
                c.start()
            greet(n)

        for step in sorted({p[0] for p in plan}):

            @pl.when(i == step)
            def _(step=step):
                for when, action, which in plan:
                    if when == step:
                        getattr(flows[which], action)()

        if not last:
            out = pltpu.make_async_copy(up_term, up_out, out_sem.at[0])

            @pl.when(i == low)
            def _():
                out.start()

            @pl.when(i == steps - 1)
            def _():
                out.wait()

        @pl.when(i < low)
        def _():
            @pl.when(lax.rem(i, tiles) == 0)
            def _():
                acc[...] = jnp.zeros_like(acc)

            acc[...] += nn(at_ref[...], dg_ref[...])

        for step, whole in ((middle - 1, gate_term), (low - 1, up_term)):

            @pl.when(i == step)
            def _(whole=whole):
                whole[...] = acc[...].astype(BF16)

        @pl.when(i == low)
        def _():
            for c in weights:
                c.wait()

        @pl.when(i >= low)
        def _():
            @pl.loop(0, bt // inner)
            def _(part):
                rows = pl.ds(pl.multiple_of(part * inner, inner), inner)
                da = (nt(dg_ref[rows, :], wg[...]) + nt(du_ref[rows, :], wu[...])).astype(BF16).astype(F32)
                wide = h_ref[rows, :].astype(F32)
                scale = scale_of(wide)
                along = jnp.mean(da * wide, -1, keepdims=True)
                dh = da * scale - wide * (scale * scale * scale * along)
                o_ref[rows, :] = dy_ref[rows, :] + dh.astype(BF16)

        if last:

            @pl.when(i == steps - 1)
            def _():
                flows[2].end()

    def late(i):
        return (jnp.maximum(i - low, 0), 0)

    def shard(rows, columns):
        if last:
            return pl.BlockSpec((2, rows // n, columns), lambda i: (0, 0, 0), pipeline_mode=pl.Buffered(1))
        return pl.BlockSpec((rows // n, columns), lambda i: (0, 0), pipeline_mode=pl.Buffered(1))

    pair = (2,) if last else ()

    scratch = [
        pltpu.VMEM((d, f), F32),
        pltpu.VMEM((d, f), BF16),
        pltpu.VMEM((d, f), BF16),
        pltpu.VMEM((d, f), BF16),
        pltpu.VMEM((d, f), BF16),
        pltpu.SemaphoreType.DMA((5,)),
        pltpu.SemaphoreType.DMA((1,)),
        *Scatter.scratch((f, d), n),
        *Scatter.scratch((d, f), n, here=True),
    ]
    if last:
        scratch += Scatter.scratch((d, f), n, here=True)
    return pl.pallas_call(
        kernel,
        grid=(steps,),
        in_specs=[
            pl.BlockSpec((d, bt), lambda i: (0, lax.rem(jnp.minimum(i, low - 1), tiles))),
            pl.BlockSpec(
                (None, bt, f),
                lambda i: (jnp.where(i < low, i // tiles, 0), jnp.where(i < low, lax.rem(i, tiles), i - low), 0),
            ),
            pl.BlockSpec((None, bt, f), lambda i: (1, jnp.maximum(i - low, 0), 0)),
            pl.BlockSpec((bt, d), late),
            pl.BlockSpec((bt, d), late),
            ANY,
            ANY,
            ANY,
            *[ANY] * len(above),
        ],
        out_specs=[pl.BlockSpec((bt, d), late), shard(f, d), shard(d, f), shard(d, f) if last else ANY],
        out_shape=[
            jax.ShapeDtypeStruct((t, d), BF16),
            jax.ShapeDtypeStruct((*pair, f // n, d), BF16),
            jax.ShapeDtypeStruct((*pair, d // n, f), BF16),
            jax.ShapeDtypeStruct((*pair, d // n if last else d, f), BF16),
        ],
        scratch_shapes=scratch,
        compiler_params=pltpu.CompilerParams(
            dimension_semantics=("arbitrary",),
            vmem_limit_bytes=63 * 1024 * 1024,
            collective_id=identity,
            has_side_effects=True,
        ),
        cost_estimate=cost(8 * t * d * f, t * f * 8 + t * d * 10),
        name="back",
    )(at, both, both, h, dy, gate, up, term, *above)


def handed_on(x, bm=512):
    def kernel(x_ref, o_ref):
        o_ref[...] = x_ref[...]

    t, d = x.shape
    return pl.pallas_call(
        kernel,
        grid=(t // bm,),
        in_specs=[rows_spec(bm, d)],
        out_specs=rows_spec(bm, d),
        out_shape=jax.ShapeDtypeStruct((t, d), BF16),
        compiler_params=params(),
        cost_estimate=cost(0, t * d * 4),
        name="handed_on",
    )(x)


def solution(mesh):
    n = mesh.shape["dp"]

    def body(x, dy, w_gate, w_up, w_down):
        shape = x.shape
        x, dy = (v.reshape(v.shape[-2:]) for v in (x, dy))
        at0, g0, u0, h1, gate, up, down = forward(x, w_gate, w_up, w_down, n)
        at1, both1, dwd1 = top_layer(h1, dy, gate, up, down, 1)
        dh1, down1, gate1, dwu1 = back(n, 1, dwd1, at1, both1, h1, dy, gate, up, 1)
        both0, dwd0, up1 = low_layer(n, [dwu1], 2, g0, u0, dh1, down, 0)
        dx, downs, gates, ups = back(n, 3, dwd0, at0, both0, x, dh1, gate, up, 0, (down1, gate1, up1))
        return handed_on(dx).reshape(shape), gates, ups, downs

    seq, row = P(("rep", "dp")), P(None, "dp")
    out = P("rep", "dp")
    return jax.shard_map(
        body, mesh=mesh, in_specs=(seq, seq, row, row, row), out_specs=(seq, out, out, out), check_vma=False
    )
```
